512 devices in a mesh: pb: 8 (over y_lo, x), ka: 64 (over z, y_hi, core).
Axes of the slice: x: 4, y: 4 (y_hi: 2, y_lo: 2; y = y_hi * 2 + y_lo), z: 16, core: 2. Of those that a mesh axis runs over, the one named last changes fastest.
Arguments:
- coupling: bfloat16 [20480, 8, 2048], P('ka', 'pb'), may hold values from -0.0048828125 to 0.0048828125
- eigvec: float32 [64, 2048], P('ka'), may hold values from -0.75 to 0.75
- energies: float32 [64, 32], P('ka'), may hold values from -1 to 1
- k_coords: int32 [3, 64], replicated, may hold values from 0 to 63
- r_coords: int32 [3, 20480], P(None, 'ka'), may hold values from -12 to 12
- degeneracy: int32 [20480], P('ka'), may hold values from 1 to 8
- kq_index: int32 [64, 96], P('ka', 'pb'), may hold values from 0 to 63
- omega: float32 [96, 8], P('pb'), may hold values from 0.05 to 0.5
- phonon_modes: float32 [96, 8, 8], P('pb'), may hold values from -2 to 2
Outputs:
- sigma: float32 [64, 32], P('ka', 'pb')
The draws below stay inside these ranges and needn't reach their ends.
All inputs are finite; a program needn't handle non-finite values.
Results may differ from the reference program's by a relative error of at most 0.0013.
Values may be sent and summed in bfloat16 or wider, within the bound.
A program may use at most 64 MiB of HBM per device.

```python
import math
import jax
import jax.numpy as jnp
from jax import lax

NB = 32
KGRID = 64
RMAX = 12
NR = 20480
MODES = 8
KTOT = 64
QTOT = 96


def place_ends(entries, stream_key, smallest, high):
    extent = entries.shape
    spot = [jax.random.randint(jax.random.fold_in(stream_key, axis), (), 0, extent[axis]) for axis in range(len(extent))]
    entries = entries.at[tuple(spot)].set(smallest)
    longest = extent.index(max(extent))
    spot[longest] = (spot[longest] + 1) % extent[longest]
    return entries.at[tuple(spot)].set(high)


def block_levels(key, shape, split, low, largest):
    factor_of, own = 1.0, jax.random.fold_in(key, 6)
    for position, parts in split:
        steps = jnp.exp(jax.random.uniform(jax.random.fold_in(own, position), (parts,), jnp.float32, low / len(split), largest / len(split)))
        factor_of = factor_of * jnp.repeat(steps, shape[position] // parts).reshape([-1 if axis == position else 1 for axis in range(len(shape))])
    return factor_of


def normal_values(rng, extent, spread, reach, shards=(), kind=jnp.bfloat16):
    result = jax.random.normal(rng, extent, jnp.float32) * spread
    if len(shards) > 0:
        result = block_levels(rng, extent, shards, -0.22, 0.18) * result
    return jnp.clip(result, min=-reach, max=reach).astype(kind)


def setup_inputs(seed: int = 0) -> dict:
    seeds = jax.random.split(jax.random.key(seed), 10)
    coupling = normal_values(seeds[0], (NR, MODES, 2 * NB * NB), (NR * 64) ** -0.5, 0.0048828125, ((0, 64), (1, 8)))
    eigvec = normal_values(seeds[1], (KTOT, 2 * NB * NB), (2 * NB) ** -0.5, 0.75, ((0, 64),), jnp.float32)
    energies = jnp.clip(jax.random.uniform(seeds[2], (KTOT, NB), jnp.float32, -1.0, 1.0) * block_levels(seeds[2], (KTOT, NB), ((0, 64),), -0.4, 0.0), -1.0, 1.0)
    k_coords = place_ends(jax.random.randint(seeds[3], (3, KTOT), 0, KGRID), jax.random.fold_in(seeds[3], 1), 0, KGRID - 1).astype(jnp.int32)
    r_coords = place_ends(jax.random.randint(seeds[4], (3, NR), 0 - RMAX, RMAX + 1), jax.random.fold_in(seeds[4], 1), 0 - RMAX, RMAX).astype(jnp.int32)
    degeneracy = place_ends(jax.random.randint(seeds[5], (NR,), 1, 9), jax.random.fold_in(seeds[5], 1), 1, 8).astype(jnp.int32)
    kq_index = place_ends(jax.random.randint(seeds[6], (KTOT, QTOT), 0, KTOT), jax.random.fold_in(seeds[6], 1), 0, KTOT - 1).astype(jnp.int32)
    omega = jnp.clip(jnp.exp(math.log(0.5) - 2.3025851 * jax.random.uniform(seeds[7], (QTOT, MODES), jnp.float32) ** block_levels(seeds[7], (QTOT, MODES), ((0, 8),), -0.2, 0.2)), 0.05, 0.5)
    phonon_modes = normal_values(seeds[8], (QTOT, MODES, MODES), MODES ** -0.5, 2.0, ((0, 8),), jnp.float32)
    return {"coupling": coupling, "eigvec": eigvec, "energies": energies, "k_coords": k_coords, "r_coords": r_coords, "degeneracy": degeneracy, "kq_index": kq_index, "omega": omega, "phonon_modes": phonon_modes}


THERMAL = 0.1
SMEARING = 0.05
HIGHEST = lax.Precision.HIGHEST


def phases(k_coords, r_coords, degeneracy):
    turns = (k_coords[0][:, None] * r_coords[0][None, :] + k_coords[1][:, None] * r_coords[1][None, :] + k_coords[2][:, None] * r_coords[2][None, :]) % KGRID
    angle = turns.astype(jnp.float32) * (2.0 * math.pi / KGRID)
    inverse = 1.0 / degeneracy.astype(jnp.float32)
    cosine = (jnp.cos(angle) * inverse[None, :]).astype(jnp.bfloat16)
    sine = (jnp.sin(angle) * inverse[None, :]).astype(jnp.bfloat16)
    return cosine, sine


def combine_parts(cosine_sum, sine_sum, modes, square):
    cosine_rows = cosine_sum.reshape(cosine_sum.shape[0], modes, 2, square)
    sine_rows = sine_sum.reshape(sine_sum.shape[0], modes, 2, square)
    real_part = cosine_rows[:, :, 0] - sine_rows[:, :, 1]
    imag_part = cosine_rows[:, :, 1] + sine_rows[:, :, 0]
    return jnp.stack([real_part, imag_part], axis=2).reshape(cosine_sum.shape[0], modes * 2 * square)


def lorentz(spacing):
    return SMEARING / (math.pi * (spacing * spacing + SMEARING * SMEARING))


def self_energy(wannier, vector, energy, kq_vectors, kq_energies, omega, phonon):
    bands = energy.shape[0]
    modes = wannier.shape[0]
    matrix = wannier.astype(jnp.float32).reshape(modes, 2, bands, bands)
    rotate = vector.reshape(2, bands, bands)
    fold_real = jnp.einsum("vac,cn->van", matrix[:, 0], rotate[0], precision=HIGHEST) - jnp.einsum("vac,cn->van", matrix[:, 1], rotate[1], precision=HIGHEST)
    fold_imag = jnp.einsum("vac,cn->van", matrix[:, 0], rotate[1], precision=HIGHEST) + jnp.einsum("vac,cn->van", matrix[:, 1], rotate[0], precision=HIGHEST)
    mixed_real = jnp.einsum("qwv,wan->qvan", phonon, fold_real, precision=HIGHEST)
    mixed_imag = jnp.einsum("qwv,wan->qvan", phonon, fold_imag, precision=HIGHEST)
    target = kq_vectors.reshape(-1, 2, bands, bands)
    final_real = jnp.einsum("qam,qvan->qmvn", target[:, 0], mixed_real, precision=HIGHEST) + jnp.einsum("qam,qvan->qmvn", target[:, 1], mixed_imag, precision=HIGHEST)
    final_imag = jnp.einsum("qam,qvan->qmvn", target[:, 0], mixed_imag, precision=HIGHEST) - jnp.einsum("qam,qvan->qmvn", target[:, 1], mixed_real, precision=HIGHEST)
    strength = final_real * final_real + final_imag * final_imag
    fermi = 1.0 / (1.0 + jnp.exp(kq_energies / THERMAL))
    bose = 1.0 / jnp.expm1(omega / THERMAL)
    spacing = energy[None, None, None, :] - kq_energies[:, :, None, None]
    absorb = lorentz(spacing + omega[:, None, :, None])
    emit = lorentz(spacing - omega[:, None, :, None])
    bose_wide = bose[:, None, :, None]
    fermi_wide = fermi[:, :, None, None]
    occupy = (bose_wide + fermi_wide) * absorb + (bose_wide + 1.0 - fermi_wide) * emit
    return jnp.sum(strength * occupy, axis=(0, 1, 2))


def reference(coupling, eigvec, energies, k_coords, r_coords, degeneracy, kq_index, omega, phonon_modes):
    cosine, sine = phases(k_coords, r_coords, degeneracy)
    flat = coupling.reshape(coupling.shape[0], -1)
    cosine_sum = jnp.dot(cosine, flat, preferred_element_type=jnp.float32)
    sine_sum = jnp.dot(sine, flat, preferred_element_type=jnp.float32)
    wannier = combine_parts(cosine_sum, sine_sum, MODES, NB * NB).astype(jnp.bfloat16)
    wannier = wannier.reshape(KTOT, MODES, 2 * NB * NB)

    def per_point(items):
        wannier_row, vector, energy, kq_row = items
        kq_vectors = eigvec[kq_row]
        kq_energies = energies[kq_row]
        return self_energy(wannier_row, vector, energy, kq_vectors, kq_energies, omega, phonon_modes)

    sigma = lax.map(per_point, (wannier, eigvec, energies, kq_index))
    return sigma / QTOT
```

```python
import functools
import math

import jax
import jax.numpy as jnp
from jax import lax
from jax.experimental import pallas as pl
from jax.experimental.pallas import tpu as pltpu
from jax.sharding import PartitionSpec as P

THERMAL = 0.1
SMEARING = 0.05
NB = 32
LANES = 128
SLOTS = 16
V_EARLY = 16
MESH = pl.DeviceIdType.MESH
BF = jnp.bfloat16
F32 = jnp.float32


def iota(shape, dim):
    return lax.broadcasted_iota(jnp.int32, shape, dim)


def spin(x, shift):
    shift = shift % LANES
    return x if shift == 0 else pltpu.roll(x, shift, 1)


def pieces(x, count):
    out = []
    for _ in range(count):
        part = x.astype(BF)
        out.append(part)
        x = x - part.astype(F32)
    return out


def body(
    np_, ka, ql,
    coup, vec, ener, kc, rc, deg, kq, om, ph,
    out,
    xbuf, sums, sendc, recvc, sendz, recvz, vsend, vgot, esend, egot,
    flat, posend, pogot, kqsend, kqgot, kqs, spread, phx, fold, fsend, fgot,
    turned, vq, occ, eq,
    xsem, csem, zsend, zrecv, vs_sem, vr_sem, es_sem, er_sem, wsem,
    ps_sem, pr_sem, ks_sem, kr_sem, ksm, fs_sem, fr_sem,
):
    ni = ka // 2
    nz = ni // 2
    nb = NB // np_
    rows = 2 * nb
    queries = ql * np_
    width = queries * NB
    tiles = width // LANES
    rl = coup.shape[0]
    me = lax.axis_index("ka")
    mp = lax.axis_index("pb")
    mc = lax.rem(me, 2)
    mi = me // 2
    mz = mi // 2
    my = lax.rem(mi, 2)
    other = {"ka": mi * 2 + (1 - mc)}

    def chip(o):
        s = o // 2
        dz = nz // 2 + ((s + 1) // 2) * (1 - 2 * lax.rem(s, 2))
        z = lax.rem(mz + dz + nz, nz)
        y = lax.rem(my + 1 - lax.rem(o, 2), 2)
        return z * 2 + y

    def mate(o):
        return lax.rem(mp + 1 + o, np_)

    def each(count, f):
        def step(o, carry):
            f(o)
            return carry
        lax.fori_loop(0, count, step, 0)

    barrier = pltpu.get_barrier_semaphore()
    each(ni - 1, lambda o: pl.semaphore_signal(
        barrier, inc=1, device_id={"ka": chip(o) * 2 + mc}, device_id_type=MESH))
    pl.semaphore_signal(barrier, inc=1, device_id=other, device_id_type=MESH)
    each(np_ - 1, lambda o: pl.semaphore_signal(
        barrier, inc=1, device_id={"pb": mate(o)}, device_id_type=MESH))

    load = pltpu.make_async_copy(coup, xbuf, xsem)
    load.start()

    kpad = jnp.concatenate(
        [kc[...].astype(F32), jnp.zeros((5, ka), F32)], axis=0)
    if ka < LANES:
        kpad = jnp.concatenate([kpad, jnp.zeros((8, LANES - ka), F32)], axis=1)
    kcol = jnp.transpose(jnp.concatenate([kpad, jnp.zeros((LANES - 8, LANES), F32)], axis=0))[:ka]
    rrow = rc[...].astype(F32)
    turns = (kcol[:, 0:1] * rrow[0:1, :] + kcol[:, 1:2] * rrow[1:2, :]) + kcol[:, 2:3] * rrow[2:3, :]
    x = turns - 64.0 * jnp.floor(turns * (1.0 / 64.0))
    quad = jnp.floor((x + 8.0) * (1.0 / 16.0))
    a = (x - 16.0 * quad) * (2.0 * math.pi / 64.0)
    a2 = a * a
    sin_a = a + a * a2 * (-1.0 / 6 + a2 * (1.0 / 120 + a2 * (-1.0 / 5040 + a2 * (1.0 / 362880))))
    cos_a = 1.0 + a2 * (-0.5 + a2 * (1.0 / 24 + a2 * (-1.0 / 720 + a2 * (1.0 / 40320))))
    odd = (quad == 1.0) | (quad == 3.0)
    cosine = jnp.where(odd, sin_a, cos_a)
    sine = jnp.where(odd, cos_a, sin_a)
    cosine = jnp.where((quad == 1.0) | (quad == 2.0), -cosine, cosine)
    sine = jnp.where((quad == 2.0) | (quad == 3.0), -sine, sine)
    inverse = 1.0 / deg[...].astype(F32)
    both = jnp.concatenate([cosine * inverse, sine * inverse], axis=0).astype(BF)

    load.wait()
    cut = min(256, rl)

    def product(at):
        total = jnp.dot(both[:, :cut], xbuf[:cut, at : at + 256], preferred_element_type=F32)
        if rl > cut:
            total += jnp.dot(both[:, cut:], xbuf[cut:, at : at + 256], preferred_element_type=F32)
        return total

    for j in range(4):
        re, im = product(256 * j), product(1024 + 256 * j)
        real = re[:ka] - im[ka:]
        imag = im[:ka] + re[ka:]
        for h in range(2):
            t = 2 * j + h
            sums[t * ka : (t + 1) * ka, :] = real[:, h * LANES : (h + 1) * LANES]
            sums[(8 + t) * ka : (9 + t) * ka, :] = imag[:, h * LANES : (h + 1) * LANES]

    def of_point(k):
        return sums[pl.ds(k, 16, stride=ka), :]

    def to_partner(i):
        sendc[i] = of_point(2 * i + (1 - mc)).astype(BF)
    each(ni, to_partner)

    lane8 = iota((8, LANES), 1)
    v = vec[...]
    vsend[...] = v.astype(BF)
    flat[...] = jnp.zeros_like(flat)
    flat[0:1, 0:NB] = ener[...]
    erow = flat[0:8, :]
    erow = (erow + spin(erow, 32)) + (spin(erow, 64) + spin(erow, 96))
    esend[...] = erow[0:1, :]
    flat[0:1, 0:NB] = jnp.zeros((1, NB), F32)
    flat[0 : np_ * np_, 0:ql] = ph[...]
    flat[64 : 64 + np_, 0:ql] = om[...]
    posend[...] = jnp.transpose(flat[...])[:SLOTS]
    kqsend[...] = jnp.zeros_like(kqsend)
    kqsend[0:1, 0:ql] = kq[...]

    pl.semaphore_wait(barrier, ni + np_ - 1)

    def copy(src, dst, s, r, to):
        return pltpu.make_async_remote_copy(
            src_ref=src, dst_ref=dst, send_sem=s, recv_sem=r, device_id=to, device_id_type=MESH)

    swap = copy(sendc, recvc, csem.at[0], csem.at[1], other)
    swap.start()

    def po_copy(o, to):
        return copy(posend, pogot.at[mp], ps_sem.at[o], pr_sem.at[mp], {"pb": to})

    def kq_copy(o, to):
        return copy(kqsend, kqgot.at[mp], ks_sem.at[o], kr_sem.at[mp], {"pb": to})

    def small(o):
        po_copy(o, mate(o)).start()
        kq_copy(o, mate(o)).start()
    each(np_ - 1, small)
    pogot[mp] = posend[...]
    kqgot[mp] = kqsend[...]

    def e_copy(o, i):
        return copy(esend, egot.at[mc, mi], es_sem.at[o], er_sem.at[mi], {"ka": i * 2 + mc})

    def v_copy(o, i):
        return copy(vsend, vgot.at[mc, mi], vs_sem.at[o], vr_sem.at[mi], {"ka": i * 2 + mc})

    def z_copy(o, i):
        return copy(sendz.at[i], recvz.at[mi], zsend.at[o], zrecv.at[mi], {"ka": i * 2 + mc})

    early = min(V_EARLY, ni - 1)

    def first(o):
        v_copy(o, chip(o)).start()
    each(early, first)
    each(ni - 1, lambda o: e_copy(o, chip(o)).start())
    vgot[mc, mi] = vsend[...]
    egot[mc, mi] = esend[...]

    swap.wait_recv()

    def add_and_send(o):
        i = chip(o)
        sendz[i] = (of_point(2 * i + mc) + recvc[i].astype(F32)).astype(BF)
        z_copy(o, i).start()
    each(ni - 1, add_and_send)
    own = of_point(me) + recvc[mi].astype(F32)

    def late(o):
        v_copy(o + early, chip(o + early)).start()
    each(ni - 1 - early, late)

    for blk, (s0, c0, s1, c1) in enumerate(
        [(1, 0, 1, 1), (-1, 1, 1, 0), (1, 1, -1, 0), (1, 0, 1, 1)]
    ):
        for low in range(4):
            left = s0 * spin(v[8 * c0 : 8 * c0 + 8], -32 * low)
            right = s1 * spin(v[8 * c1 : 8 * c1 + 8], 32 - 32 * low)
            val = jnp.where(lane8 < 32, left, jnp.where(lane8 < 64, right, 0.0))
            flat[pl.ds(32 * blk + low, 8, stride=4), :] = val
    table = jnp.transpose(flat[...])[:64]
    r_at, c_at = iota((64, 64), 0), iota((64, 64), 1)
    pick = (((r_at // nb) % 2) * NB + (r_at // rows) * nb + r_at % nb == c_at).astype(F32).astype(BF)
    for h, part in enumerate(pieces(table, 2)):
        fold[:, h * LANES : (h + 1) * LANES] = jnp.dot(
            pick, part, preferred_element_type=F32).astype(BF)

    q_at = iota((LANES, width), 1) // NB
    spread[...] = ((q_at // ql) * SLOTS + q_at % ql == iota((LANES, width), 0)).astype(F32).astype(BF)

    def small_wait(o):
        src = mate(o)
        po_in = copy(posend, pogot.at[src], ps_sem.at[o], pr_sem.at[src], {"pb": src})
        po_in.wait_recv()
        kq_in = copy(kqsend, kqgot.at[src], ks_sem.at[o], kr_sem.at[src], {"pb": src})
        kq_in.wait_recv()
    each(np_ - 1, small_wait)
    to_scalar = pltpu.make_async_copy(kqgot, kqs, ksm)
    to_scalar.start()
    got = pogot[...].reshape(np_ * SLOTS, LANES)
    if np_ * SLOTS < LANES:
        got = jnp.concatenate([got, jnp.zeros((LANES - np_ * SLOTS, LANES), F32)], axis=0)
    three = pieces(jnp.transpose(got)[:72], 3)
    three = [jnp.concatenate([p.astype(F32), jnp.zeros((8, LANES), F32)], axis=0).astype(BF) for p in three]
    for j in range(width // 256 if width % 256 == 0 else 0):
        at = slice(256 * j, 256 * j + 256)
        total = jnp.dot(three[0], spread[:, at], preferred_element_type=F32)
        total += jnp.dot(three[1], spread[:, at], preferred_element_type=F32)
        total += jnp.dot(three[2], spread[:, at], preferred_element_type=F32)
        phx[:, at] = total
    to_scalar.wait()

    def z_wait(o, total):
        i = chip(o)
        copy(sendz.at[i], recvz.at[i], zsend.at[o], zrecv.at[i], {"ka": i * 2 + mc}).wait_recv()
        return total + recvz[i].astype(F32)
    wann = lax.fori_loop(0, ni - 1, z_wait, own).astype(BF).astype(F32)
    blocks = []
    for low in range(4):
        for part in range(2):
            at = 64 * part
            w0 = spin(wann[0:8], at - 32 * low)
            w1 = spin(wann[8:16], at + 32 - 32 * low)
            blocks.append(jnp.where(
                (lane8 >= at) & (lane8 < at + 32), w0,
                jnp.where((lane8 >= at + 32) & (lane8 < at + 64), w1, 0.0)))
    right = jnp.concatenate(blocks + [jnp.zeros((64, LANES), F32)], axis=0).astype(BF)
    right = jnp.concatenate([right, right], axis=1)
    folded = lax.dot_general(
        fold[...], right, (((1,), (1,)), ((), ())), preferred_element_type=F32)
    for p in range(np_):
        fsend[p] = folded[p * rows : (p + 1) * rows]

    def f_copy(o, to):
        return copy(fsend.at[to], fgot.at[mp], fs_sem.at[o], fr_sem.at[mp], {"pb": to})
    each(np_ - 1, lambda o: f_copy(o, mate(o)).start())
    fgot[mp] = fsend[mp]

    def v_wait(o):
        i = chip(o)
        copy(vsend, vgot.at[mc, i], vs_sem.at[o], vr_sem.at[i], {"ka": i * 2 + mc}).wait_recv()
        copy(esend, egot.at[mc, i], es_sem.at[o], er_sem.at[i], {"ka": i * 2 + mc}).wait_recv()
    each(ni - 1, v_wait)
    give_v = copy(vgot.at[mc], vgot.at[mc], wsem.at[0], wsem.at[1], other)
    give_e = copy(egot.at[mc], egot.at[mc], wsem.at[2], wsem.at[3], other)
    give_v.start()
    give_e.start()

    def rolled(c):
        def step(i):
            val = vgot[c, i].astype(F32)
            turned[0, c, i] = val
            for s in range(1, 4):
                turned[s, c, i] = spin(val, 32 * s)
        each(ni, step)
    rolled(mc)
    copy(vgot.at[1 - mc], vgot.at[1 - mc], wsem.at[0], wsem.at[1], other).wait_recv()
    copy(egot.at[1 - mc], egot.at[1 - mc], wsem.at[2], wsem.at[3], other).wait_recv()
    rolled(1 - mc)

    lane16 = iota((16, LANES), 1) // NB
    lane1 = iota((1, LANES), 1) // NB
    row_e = iota((rows, LANES), 0) % nb + mp * nb
    e_col = jnp.sum(
        jnp.where(iota((rows, LANES), 1) == row_e, esend[...], 0.0), axis=1, keepdims=True)

    def by_group(mask, vals):
        return jnp.where(mask == 0, vals[0], jnp.where(
            mask == 1, vals[1], jnp.where(mask == 2, vals[2], vals[3])))

    def tables(t):
        at = pl.ds(pl.multiple_of(t * LANES, LANES), LANES)
        where = []
        for g in range(4):
            q = 4 * t + g
            point = kqs[q // ql, 0, lax.rem(q, ql)]
            where.append((lax.rem(point, 2), point // 2))
        for low in range(4):
            vq[16 * low : 16 * low + 16, at] = by_group(
                lane16, [turned[(g - low) % 4, where[g][0], where[g][1]] for g in range(4)]).astype(BF)
        e_there = by_group(lane1, [egot[where[g][0], where[g][1]] for g in range(4)])
        fermi = 1.0 / (1.0 + jnp.exp(e_there * (1.0 / THERMAL)))
        gap = e_col - e_there
        omega = phx[64:72, at]
        bose = 1.0 / (jnp.exp(omega * (1.0 / THERMAL)) - 1.0)
        for m in range(np_):
            w, b = omega[m : m + 1], bose[m : m + 1]
            up, down = gap + w, gap - w
            scale = SMEARING / (math.pi * queries)
            value = (b + fermi) * (scale / (up * up + SMEARING * SMEARING))
            value += (b + 1.0 - fermi) * (scale / (down * down + SMEARING * SMEARING))
            occ[m, :, at] = value
    each(tiles, tables)

    def f_wait(o):
        src = mate(o)
        copy(fsend.at[src], fgot.at[src], fs_sem.at[o], fr_sem.at[src], {"pb": src}).wait_recv()
    each(np_ - 1, f_wait)
    left = fgot[...].reshape(np_ * rows, LANES)[:, :64].astype(BF)

    def finish(t, total):
        at = pl.ds(pl.multiple_of(t * 256, 256), 256)
        h = jnp.dot(left, vq[:, at], preferred_element_type=F32)
        for m in range(np_):
            g = phx[m : m + 1, at] * h[0:rows]
            for w in range(1, np_):
                g += phx[w * np_ + m : w * np_ + m + 1, at] * h[w * rows : (w + 1) * rows]
            total += (g * g) * occ[m, :, at]
        return total
    total = lax.fori_loop(0, width // 256, finish, jnp.zeros((rows, 256), F32))
    summed = jnp.sum(total, axis=1, keepdims=True)
    out[...] = jnp.sum(
        jnp.where(iota((rows, LANES), 1) == iota((rows, LANES), 0) % nb, summed, 0.0),
        axis=0, keepdims=True)[:, :nb]

    swap.wait_send()
    give_v.wait_send()
    give_e.wait_send()

    def drain(o):
        i = chip(o)
        z_copy(o, i).wait_send()
        v_copy(o, i).wait_send()
        e_copy(o, i).wait_send()
    each(ni - 1, drain)

    def drain_small(o):
        po_copy(o, mate(o)).wait_send()
        kq_copy(o, mate(o)).wait_send()
        f_copy(o, mate(o)).wait_send()
    each(np_ - 1, drain_small)


def shards(mesh, coupling, eigvec, energies, k_coords, r_coords, degeneracy, kq_index, omega, phonon_modes):
    np_, ka = mesh.shape["pb"], mesh.shape["ka"]
    rl = coupling.shape[0]
    ql = omega.shape[0]
    ni = ka // 2
    nb = NB // np_
    rows = 2 * nb
    width = ql * np_ * NB
    vm = pl.BlockSpec(memory_space=pltpu.VMEM)
    hbm = pl.BlockSpec(memory_space=pl.ANY)
    V = pltpu.VMEM
    sem = pltpu.SemaphoreType.DMA
    return pl.pallas_call(
        functools.partial(body, np_, ka, ql),
        out_shape=jax.ShapeDtypeStruct((1, nb), F32),
        in_specs=[hbm] + [vm] * 8,
        out_specs=vm,
        scratch_shapes=[
            V((rl, 2048), BF),
            V((16 * ka, LANES), F32),
            V((ni, 16, LANES), BF),
            V((ni, 16, LANES), BF),
            V((ni, 16, LANES), BF),
            V((ni, 16, LANES), BF),
            V((16, LANES), BF),
            V((2, ni, 16, LANES), BF),
            V((1, LANES), F32),
            V((2, ni, 1, LANES), F32),
            V((LANES, LANES), F32),
            V((SLOTS, LANES), F32),
            V((np_, SLOTS, LANES), F32),
            V((1, LANES), jnp.int32),
            V((np_, 1, LANES), jnp.int32),
            pltpu.SMEM((np_, 1, LANES), jnp.int32),
            V((LANES, width), BF),
            V((80, width), F32),
            V((64, 256), BF),
            V((np_, rows, LANES), F32),
            V((np_, rows, LANES), F32),
            V((4, 2, ni, 16, LANES), F32),
            V((64, width), BF),
            V((np_, rows, width), F32),
            V((1, LANES), F32),
            sem, sem((2,)), sem((ni,)), sem((ni,)), sem((ni,)), sem((ni,)), sem((ni,)), sem((ni,)), sem((4,)),
            sem((np_,)), sem((np_,)), sem((np_,)), sem((np_,)), sem, sem((np_,)), sem((np_,)),
        ],
        compiler_params=pltpu.CompilerParams(collective_id=0, has_side_effects=True),
        name="self_energy",
    )(
        coupling.reshape(rl, 2048),
        eigvec.reshape(16, LANES),
        energies,
        k_coords,
        r_coords,
        degeneracy.reshape(1, rl),
        kq_index,
        omega.T,
        jnp.transpose(phonon_modes, (1, 2, 0)).reshape(np_ * np_, ql),
    )


def solution(mesh):
    in_specs = (
        P("ka", "pb", None),
        P("ka", None),
        P("ka", None),
        P(),
        P(None, "ka"),
        P("ka"),
        P("ka", "pb"),
        P("pb", None),
        P("pb", None, None),
    )
    return jax.shard_map(
        functools.partial(shards, mesh), mesh=mesh, in_specs=in_specs,
        out_specs=P("ka", "pb"), check_vma=False)
```

```python
import functools
import math

import jax
import jax.numpy as jnp
from jax import lax
from jax.experimental import pallas as pl
from jax.experimental.pallas import tpu as pltpu
from jax.sharding import PartitionSpec as P

THERMAL = 0.1
SMEARING = 0.05
NB = 32
LANES = 128
SLOTS = 16
MESH = pl.DeviceIdType.MESH
BF = jnp.bfloat16
F32 = jnp.float32


def iota(shape, dim):
    return lax.broadcasted_iota(jnp.int32, shape, dim)


def spin(x, shift):
    shift = shift % LANES
    return x if shift == 0 else pltpu.roll(x, shift, 1)


def pieces(x, count):
    out = []
    for _ in range(count):
        part = x.astype(BF)
        out.append(part)
        x = x - part.astype(F32)
    return out


def body(
    np_, ka, ql,
    coup, vec_in, ener_in, kc_in, rc_in, deg_in, kq_in, om_in, ph_in,
    out,
    vec, ener, kc, rc, deg, kq, om, ph,
    xbuf, sums, sendc, recvc, sendz, recvz, vsend, vrows, esend, egot,
    flat, posend, pogot, kqsend, kqgot, kqs, spread, phx, fold, fsend, fgot,
    slots, shifts, raw, vq, occ, small_sem,
    xsem, csem, zsend, zrecv, vs_sem, vr_sem, es_sem, er_sem, wsem, vp_send, vp_recv,
    ps_sem, pr_sem, ks_sem, kr_sem, ksm, fs_sem, fr_sem,
):
    ni = ka // 2
    nz = ni // 2
    nb = NB // np_
    rows = 2 * nb
    queries = ql * np_
    width = queries * NB
    tiles = width // LANES
    rl = coup.shape[0]
    me = lax.axis_index("ka")
    mp = lax.axis_index("pb")
    mc = lax.rem(me, 2)
    mi = me // 2
    mz = mi // 2
    my = lax.rem(mi, 2)
    other = {"ka": mi * 2 + (1 - mc)}

    def chip(o):
        s = o // 2
        dz = nz // 2 + ((s + 1) // 2) * (1 - 2 * lax.rem(s, 2))
        z = lax.rem(mz + dz + nz, nz)
        y = lax.rem(my + 1 - lax.rem(o, 2), 2)
        return z * 2 + y

    def mate(o):
        return lax.rem(mp + 1 + o, np_)

    def each(count, f, unroll=True):
        def step(o, carry):
            f(o)
            return carry
        if count:
            lax.fori_loop(0, count, step, 0, unroll=unroll)

    barrier = pltpu.get_barrier_semaphore()
    each(ni - 1, lambda o: pl.semaphore_signal(
        barrier, inc=1, device_id={"ka": chip(o) * 2 + mc}, device_id_type=MESH))
    pl.semaphore_signal(barrier, inc=1, device_id=other, device_id_type=MESH)
    each(np_ - 1, lambda o: pl.semaphore_signal(
        barrier, inc=1, device_id={"pb": mate(o)}, device_id_type=MESH))

    loads = [pltpu.make_async_copy(src, dst, small_sem.at[n]) for n, (src, dst) in enumerate([
        (kc_in, kc), (rc_in, rc), (deg_in, deg), (vec_in, vec), (ener_in, ener), (kq_in, kq), (om_in, om), (ph_in, ph)])]
    for c in loads[:3]:
        c.start()
    load = pltpu.make_async_copy(coup, xbuf, xsem)
    load.start()
    for c in loads[3:]:
        c.start()
    for c in loads[:3]:
        c.wait()

    kpad = jnp.concatenate(
        [kc[...].astype(F32), jnp.zeros((5, ka), F32)], axis=0)
    if ka < LANES:
        kpad = jnp.concatenate([kpad, jnp.zeros((8, LANES - ka), F32)], axis=1)
    kcol = jnp.transpose(jnp.concatenate([kpad, jnp.zeros((LANES - 8, LANES), F32)], axis=0))[:ka]
    rrow = rc[...].astype(F32)
    turns = (kcol[:, 0:1] * rrow[0:1, :] + kcol[:, 1:2] * rrow[1:2, :]) + kcol[:, 2:3] * rrow[2:3, :]
    x = turns - 64.0 * jnp.floor(turns * (1.0 / 64.0))
    quad = jnp.floor((x + 8.0) * (1.0 / 16.0))
    a = (x - 16.0 * quad) * (2.0 * math.pi / 64.0)
    a2 = a * a
    sin_a = a + a * a2 * (-1.0 / 6 + a2 * (1.0 / 120 + a2 * (-1.0 / 5040 + a2 * (1.0 / 362880))))
    cos_a = 1.0 + a2 * (-0.5 + a2 * (1.0 / 24 + a2 * (-1.0 / 720 + a2 * (1.0 / 40320))))
    odd = (quad == 1.0) | (quad == 3.0)
    cosine = jnp.where(odd, sin_a, cos_a)
    sine = jnp.where(odd, cos_a, sin_a)
    cosine = jnp.where((quad == 1.0) | (quad == 2.0), -cosine, cosine)
    sine = jnp.where((quad == 2.0) | (quad == 3.0), -sine, sine)
    inverse = 1.0 / deg[...].reshape(1, rl).astype(F32)
    both = jnp.concatenate([cosine * inverse, sine * inverse], axis=0).astype(BF)

    load.wait()
    cut = min(256, rl)

    def product(at):
        total = jnp.dot(both[:, :cut], xbuf[:cut, at : at + 256], preferred_element_type=F32)
        if rl > cut:
            total += jnp.dot(both[:, cut:], xbuf[cut:, at : at + 256], preferred_element_type=F32)
        return total

    for j in range(4):
        re, im = product(256 * j), product(1024 + 256 * j)
        real = re[:ka] - im[ka:]
        imag = im[:ka] + re[ka:]
        for h in range(2):
            t = 2 * j + h
            sums[t * ka : (t + 1) * ka, :] = real[:, h * LANES : (h + 1) * LANES]
            sums[(8 + t) * ka : (9 + t) * ka, :] = imag[:, h * LANES : (h + 1) * LANES]

    def of_point(k):
        return sums[pl.ds(k, 16, stride=ka), :]

    def to_partner(i):
        sendc[i] = of_point(2 * i + (1 - mc)).astype(BF)
    each(ni, to_partner)

    for c in loads[3:]:
        c.wait()
    lane8 = iota((8, LANES), 1)
    v = vec[...]
    vsend[...] = v.astype(BF)
    flat[...] = jnp.zeros_like(flat)
    flat[0:1, 0:NB] = ener[...]
    erow = flat[0:8, :]
    erow = (erow + spin(erow, 32)) + (spin(erow, 64) + spin(erow, 96))
    esend[...] = erow[0:1, :]
    flat[0:1, 0:NB] = jnp.zeros((1, NB), F32)
    flat[0 : np_ * np_, 0:ql] = ph[...]
    flat[64 : 64 + np_, 0:ql] = om[...]
    posend[...] = jnp.transpose(flat[...])[:SLOTS]
    kqsend[...] = jnp.zeros_like(kqsend)
    kqsend[0:1, 0:ql] = kq[...]

    pl.semaphore_wait(barrier, ni + np_ - 1)

    def copy(src, dst, s, r, to):
        return pltpu.make_async_remote_copy(
            src_ref=src, dst_ref=dst, send_sem=s, recv_sem=r, device_id=to, device_id_type=MESH)

    swap = copy(sendc, recvc, csem.at[0], csem.at[1], other)
    swap.start()

    def po_copy(o, to):
        return copy(posend, pogot.at[mp], ps_sem.at[o], pr_sem.at[mp], {"pb": to})

    def kq_copy(o, to):
        return copy(kqsend, kqgot.at[mp], ks_sem.at[o], kr_sem.at[mp], {"pb": to})

    def small(o):
        po_copy(o, mate(o)).start()
        kq_copy(o, mate(o)).start()
    each(np_ - 1, small)
    pogot[mp] = posend[...]
    kqgot[mp] = kqsend[...]

    nj = ni // np_

    def e_copy(o, i):
        return copy(esend, egot.at[mc * ni + mi], es_sem.at[o], er_sem.at[mi], {"ka": i * 2 + mc})

    def v_slot(j):
        return vrows.at[mc * ni + mp * nj + j]

    def v_copy(j, i):
        return copy(vsend, v_slot(j), vs_sem.at[j], vr_sem.at[j], {"ka": i * 2 + mc})

    def z_copy(o, i):
        return copy(sendz.at[i], recvz.at[mi], zsend.at[o], zrecv.at[mi], {"ka": i * 2 + mc})

    last = mp == np_ - 1
    each(nj - 1, lambda j: v_copy(j, chip(mp + np_ * j)).start())

    @pl.when(jnp.logical_not(last))
    def _():
        v_copy(nj - 1, chip(mp + np_ * (nj - 1))).start()

    @pl.when(last)
    def _():
        vrows[mc * ni + mp * nj + nj - 1] = vsend[...]
    each(ni - 1, lambda o: e_copy(o, chip(o)).start())
    egot[mc * ni + mi] = esend[...]

    swap.wait_recv()

    def add_and_send(o):
        i = chip(o)
        sendz[i] = (of_point(2 * i + mc) + recvc[i].astype(F32)).astype(BF)
        z_copy(o, i).start()
    each(ni - 1, add_and_send)
    own = of_point(me) + recvc[mi].astype(F32)

    for blk, (s0, c0, s1, c1) in enumerate(
        [(1, 0, 1, 1), (-1, 1, 1, 0), (1, 1, -1, 0), (1, 0, 1, 1)]
    ):
        for low in range(4):
            left = s0 * spin(v[8 * c0 : 8 * c0 + 8], -32 * low)
            right = s1 * spin(v[8 * c1 : 8 * c1 + 8], 32 - 32 * low)
            val = jnp.where(lane8 < 32, left, jnp.where(lane8 < 64, right, 0.0))
            flat[pl.ds(32 * blk + low, 8, stride=4), :] = val
    table = jnp.transpose(flat[...])[:64]
    r_at, c_at = iota((64, 64), 0), iota((64, 64), 1)
    pick = (((r_at // nb) % 2) * NB + (r_at // rows) * nb + r_at % nb == c_at).astype(F32).astype(BF)
    for h, part in enumerate(pieces(table, 2)):
        fold[:, h * LANES : (h + 1) * LANES] = jnp.dot(
            pick, part, preferred_element_type=F32).astype(BF)

    q_at = iota((LANES, width), 1) // NB
    spread[...] = ((q_at // ql) * SLOTS + q_at % ql == iota((LANES, width), 0)).astype(F32).astype(BF)

    r_at, c_at = iota((512, 512), 0), iota((512, 512), 1)
    same = (r_at // LANES == (c_at // NB) % 4) & ((r_at // NB) % 4 == c_at // LANES) & (r_at % NB == c_at % NB)
    shifts[...] = same.astype(F32).astype(BF)

    def small_wait(o):
        src = mate(o)
        po_in = copy(posend, pogot.at[src], ps_sem.at[o], pr_sem.at[src], {"pb": src})
        po_in.wait_recv()
        kq_in = copy(kqsend, kqgot.at[src], ks_sem.at[o], kr_sem.at[src], {"pb": src})
        kq_in.wait_recv()
    each(np_ - 1, small_wait)
    to_scalar = pltpu.make_async_copy(kqgot, kqs, ksm)
    to_scalar.start()
    got = pogot[...].reshape(np_ * SLOTS, LANES)
    if np_ * SLOTS < LANES:
        got = jnp.concatenate([got, jnp.zeros((LANES - np_ * SLOTS, LANES), F32)], axis=0)
    three = pieces(jnp.transpose(got)[:72], 3)
    three = [jnp.concatenate([p.astype(F32), jnp.zeros((8, LANES), F32)], axis=0).astype(BF) for p in three]
    for j in range(width // 256 if width % 256 == 0 else 0):
        at = slice(256 * j, 256 * j + 256)
        total = jnp.dot(three[0], spread[:, at], preferred_element_type=F32)
        total += jnp.dot(three[1], spread[:, at], preferred_element_type=F32)
        total += jnp.dot(three[2], spread[:, at], preferred_element_type=F32)
        phx[:, at] = total
    to_scalar.wait()

    def v_arrived(j):
        copy(vsend, v_slot(j), vs_sem.at[j], vr_sem.at[j], {"ka": me}).wait_recv()

    each(nj - 1, v_arrived)

    @pl.when(jnp.logical_not(last))
    def _():
        v_arrived(nj - 1)

    def v_block(p, c):
        return vrows.at[pl.ds(c * ni + p * nj, nj)]

    def vp_copy(o, p, to):
        return copy(v_block(p, mc), v_block(p, mc), vp_send.at[o], vp_recv.at[p], {"pb": to})
    each(np_ - 1, lambda o: vp_copy(o, mp, mate(o)).start())

    def find(q):
        point = kqs[q // ql, 0, lax.rem(q, ql)]
        c, i = lax.rem(point, 2), point // 2
        dz = lax.rem(mz - i // 2 + nz, nz) - nz // 2
        dy = lax.rem(my - lax.rem(i, 2) + 2, 2)
        o = 2 * jnp.where(dz >= 0, 2 * dz, -2 * dz - 1) + 1 - dy
        slots[0, q] = c * ni + lax.rem(o, np_) * nj + o // np_
        slots[1, q] = c * ni + i
    each(queries, find, unroll=4)

    def e_wait(o):
        i = chip(o)
        copy(esend, egot.at[mc * ni + i], es_sem.at[o], er_sem.at[i], {"ka": i * 2 + mc}).wait_recv()
    each(ni - 1, e_wait)

    def e_half(c):
        return egot.at[pl.ds(c * ni, ni)]
    give_e = copy(e_half(mc), e_half(mc), wsem.at[2], wsem.at[3], other)
    give_e.start()
    copy(e_half(1 - mc), e_half(1 - mc), wsem.at[2], wsem.at[3], other).wait_recv()

    lane1 = iota((1, LANES), 1) // NB
    row_e = iota((rows, LANES), 0) % nb + mp * nb
    e_col = jnp.sum(
        jnp.where(iota((rows, LANES), 1) == row_e, esend[...], 0.0), axis=1, keepdims=True)

    def occupations(t):
        at = pl.ds(pl.multiple_of(t * LANES, LANES), LANES)
        e4 = [egot[slots[1, 4 * t + g]] for g in range(4)]
        e_there = jnp.where(lane1 < 2, jnp.where(lane1 == 0, e4[0], e4[1]), jnp.where(lane1 == 2, e4[2], e4[3]))
        fermi = 1.0 / (1.0 + jnp.exp(e_there * (1.0 / THERMAL)))
        gap = e_col - e_there
        omega = phx[64 : 64 + np_, at]
        bose = 1.0 / (jnp.exp(omega * (1.0 / THERMAL)) - 1.0)
        scale = SMEARING / (math.pi * queries)
        for m in range(np_):
            w, b = omega[m : m + 1], bose[m : m + 1]
            up, down = gap + w, gap - w
            value = (b + fermi) * (scale / (up * up + SMEARING * SMEARING))
            value += (b + 1.0 - fermi) * (scale / (down * down + SMEARING * SMEARING))
            occ[m, :, at] = value
    each(tiles, occupations, unroll=2)

    def z_wait(o, total):
        i = chip(o)
        copy(sendz.at[i], recvz.at[i], zsend.at[o], zrecv.at[i], {"ka": i * 2 + mc}).wait_recv()
        return total + recvz[i].astype(F32)
    wann = lax.fori_loop(0, ni - 1, z_wait, own, unroll=True).astype(BF).astype(F32)
    blocks = []
    for low in range(4):
        for part in range(2):
            at = 64 * part
            w0 = spin(wann[0:8], at - 32 * low)
            w1 = spin(wann[8:16], at + 32 - 32 * low)
            blocks.append(jnp.where(
                (lane8 >= at) & (lane8 < at + 32), w0,
                jnp.where((lane8 >= at + 32) & (lane8 < at + 64), w1, 0.0)))
    right = jnp.concatenate(blocks + [jnp.zeros((64, LANES), F32)], axis=0).astype(BF)
    right = jnp.concatenate([right, right], axis=1)
    folded = lax.dot_general(
        fold[...], right, (((1,), (1,)), ((), ())), preferred_element_type=F32)
    for p in range(np_):
        fsend[p] = folded[p * rows : (p + 1) * rows]

    def f_copy(o, to):
        return copy(fsend.at[to], fgot.at[mp], fs_sem.at[o], fr_sem.at[mp], {"pb": to})
    each(np_ - 1, lambda o: f_copy(o, mate(o)).start())
    fgot[mp] = fsend[mp]

    def vp_wait(o):
        src = mate(o)
        vp_copy(o, src, src).wait_recv()
    each(np_ - 1, vp_wait)

    def v_half(c):
        return vrows.at[pl.ds(c * ni, ni)]
    give_v = copy(v_half(mc), v_half(mc), wsem.at[0], wsem.at[1], other)
    give_v.start()

    swap.wait_send()
    give_e.wait_send()

    def drain(o):
        i = chip(o)
        z_copy(o, i).wait_send()
        e_copy(o, i).wait_send()
    each(ni - 1, drain)
    each(nj - 1, lambda j: v_copy(j, chip(mp + np_ * j)).wait_send())

    @pl.when(jnp.logical_not(last))
    def _():
        v_copy(nj - 1, chip(mp + np_ * (nj - 1))).wait_send()

    def drain_small(o):
        po_copy(o, mate(o)).wait_send()
        kq_copy(o, mate(o)).wait_send()
        vp_copy(o, mp, mate(o)).wait_send()
    each(np_ - 1, drain_small)

    copy(v_half(1 - mc), v_half(1 - mc), wsem.at[0], wsem.at[1], other).wait_recv()

    def take(t):
        for g in range(4):
            raw[pl.ds(pl.multiple_of(t * 16, 16), 16), g * LANES : (g + 1) * LANES] = vrows[slots[0, 4 * t + g]]
    each(tiles, take, unroll=4)
    for h in range(2):
        moved = jnp.dot(raw[...], shifts[:, 256 * h : 256 * h + 256], preferred_element_type=F32).astype(BF)
        for low in range(2):
            for t in range(tiles):
                vq[32 * h + 16 * low : 32 * h + 16 * low + 16, t * LANES : (t + 1) * LANES] = moved[
                    16 * t : 16 * t + 16, low * LANES : (low + 1) * LANES]

    def f_wait(o):
        src = mate(o)
        copy(fsend.at[src], fgot.at[src], fs_sem.at[o], fr_sem.at[src], {"pb": src}).wait_recv()
    each(np_ - 1, f_wait)
    left = fgot[...].reshape(np_ * rows, LANES)[:, :64].astype(BF)

    def finish(t, total):
        at = pl.ds(pl.multiple_of(t * 256, 256), 256)
        h = jnp.dot(left, vq[:, at], preferred_element_type=F32)
        for m in range(np_):
            g = phx[m : m + 1, at] * h[0:rows]
            for w in range(1, np_):
                g += phx[w * np_ + m : w * np_ + m + 1, at] * h[w * rows : (w + 1) * rows]
            total += (g * g) * occ[m, :, at]
        return total
    total = lax.fori_loop(0, width // 256, finish, jnp.zeros((rows, 256), F32), unroll=True)
    summed = jnp.sum(total, axis=1, keepdims=True)
    out[...] = jnp.sum(
        jnp.where(iota((rows, LANES), 1) == iota((rows, LANES), 0) % nb, summed, 0.0),
        axis=0, keepdims=True)[:, :nb]

    give_v.wait_send()
    each(np_ - 1, lambda o: f_copy(o, mate(o)).wait_send())


def shards(mesh, coupling, eigvec, energies, k_coords, r_coords, degeneracy, kq_index, omega, phonon_modes):
    np_, ka = mesh.shape["pb"], mesh.shape["ka"]
    rl = coupling.shape[0]
    ql = omega.shape[0]
    ni = ka // 2
    nb = NB // np_
    rows = 2 * nb
    width = ql * np_ * NB
    vm = pl.BlockSpec(memory_space=pltpu.VMEM)
    hbm = pl.BlockSpec(memory_space=pl.ANY)
    V = pltpu.VMEM
    sem = pltpu.SemaphoreType.DMA
    return pl.pallas_call(
        functools.partial(body, np_, ka, ql),
        out_shape=jax.ShapeDtypeStruct((1, nb), F32),
        in_specs=[hbm] * 9,
        out_specs=vm,
        scratch_shapes=[
            V((16, LANES), F32),
            V((1, NB), F32),
            V((3, ka), jnp.int32),
            V((3, rl), jnp.int32),
            V((rl,), jnp.int32),
            V((1, ql), jnp.int32),
            V((np_, ql), F32),
            V((np_ * np_, ql), F32),
            V((rl, 2048), BF),
            V((16 * ka, LANES), F32),
            V((ni, 16, LANES), BF),
            V((ni, 16, LANES), BF),
            V((ni, 16, LANES), BF),
            V((ni, 16, LANES), BF),
            V((16, LANES), BF),
            V((2 * ni, 16, LANES), BF),
            V((1, LANES), F32),
            V((2 * ni, 1, LANES), F32),
            V((LANES, LANES), F32),
            V((SLOTS, LANES), F32),
            V((np_, SLOTS, LANES), F32),
            V((1, LANES), jnp.int32),
            V((np_, 1, LANES), jnp.int32),
            pltpu.SMEM((np_, 1, LANES), jnp.int32),
            V((LANES, width), BF),
            V((80, width), F32),
            V((64, 256), BF),
            V((np_, rows, LANES), F32),
            V((np_, rows, LANES), F32),
            pltpu.SMEM((2, ql * np_), jnp.int32),
            V((512, 512), BF),
            V((width // 8, 512), BF),
            V((64, width), BF),
            V((np_, rows, width), F32),
            sem((8,)),
            sem, sem((2,)), sem((ni,)), sem((ni,)), sem((ni,)), sem((ni,)), sem((ni,)), sem((ni,)), sem((4,)), sem((np_,)), sem((np_,)),
            sem((np_,)), sem((np_,)), sem((np_,)), sem((np_,)), sem, sem((np_,)), sem((np_,)),
        ],
        compiler_params=pltpu.CompilerParams(collective_id=0, has_side_effects=True),
        name="self_energy",
    )(
        coupling.reshape(rl, 2048),
        eigvec.reshape(16, LANES),
        energies,
        k_coords,
        r_coords,
        degeneracy,
        kq_index,
        omega.T,
        jnp.transpose(phonon_modes, (1, 2, 0)).reshape(np_ * np_, ql),
    )


def solution(mesh):
    in_specs = (
        P("ka", "pb", None),
        P("ka", None),
        P("ka", None),
        P(),
        P(None, "ka"),
        P("ka"),
        P("ka", "pb"),
        P("pb", None),
        P("pb", None, None),
    )
    return jax.shard_map(
        functools.partial(shards, mesh), mesh=mesh, in_specs=in_specs,
        out_specs=P("ka", "pb"), check_vma=False)
```

```python
import functools
import math

import jax
import jax.numpy as jnp
from jax import lax
from jax.experimental import pallas as pl
from jax.experimental.pallas import tpu as pltpu
from jax.sharding import PartitionSpec as P

THERMAL = 0.1
SMEARING = 0.05
NB = 32
LANES = 128
SLOTS = 16
MESH = pl.DeviceIdType.MESH
BF = jnp.bfloat16
F32 = jnp.float32


def iota(shape, dim):
    return lax.broadcasted_iota(jnp.int32, shape, dim)


def spin(x, shift):
    shift = shift % LANES
    return x if shift == 0 else pltpu.roll(x, shift, 1)


def pieces(x, count):
    out = []
    for _ in range(count):
        part = x.astype(BF)
        out.append(part)
        x = x - part.astype(F32)
    return out


def body(
    np_, ka, ql,
    coup, vec_in, ener_in, kc_in, rc_in, deg_in, kq_in, om_in, ph_in,
    out,
    vec, ener, kc, rc, deg, kq, om, ph,
    xbuf, sums, sendc, recvc, sendz, recvz, vsend, vrows, esend, egot,
    flat, posend, pogot, kqsend, kqgot, kqs, spread, phx, fold, fsend, fgot,
    slots, shifts, raw, vq, occ, small_sem,
    xsem, csem, wsem, ksm, sems,
):
    ni = ka // 2
    nz = ni // 2
    nb = NB // np_
    rows = 2 * nb
    queries = ql * np_
    width = queries * NB
    tiles = width // LANES
    rl = coup.shape[0]
    me = lax.axis_index("ka")
    mp = lax.axis_index("pb")
    mc = lax.rem(me, 2)
    mi = me // 2
    mz = mi // 2
    my = lax.rem(mi, 2)
    other = {"ka": mi * 2 + (1 - mc)}

    def chip(o):
        s = o // 2
        dz = nz // 2 + ((s + 1) // 2) * (1 - 2 * lax.rem(s, 2))
        z = lax.rem(mz + dz + nz, nz)
        y = lax.rem(my + 1 - lax.rem(o, 2), 2)
        return z * 2 + y

    def mate(o):
        return lax.rem(mp + 1 + o, np_)

    def each(count, f, unroll=True):
        def step(o, carry):
            f(o)
            return carry
        if count:
            lax.fori_loop(0, count, step, 0, unroll=unroll)

    barrier = pltpu.get_barrier_semaphore()
    each(ni - 1, lambda o: pl.semaphore_signal(
        barrier, inc=1, device_id={"ka": chip(o) * 2 + mc}, device_id_type=MESH))
    pl.semaphore_signal(barrier, inc=1, device_id=other, device_id_type=MESH)
    each(np_ - 1, lambda o: pl.semaphore_signal(
        barrier, inc=1, device_id={"pb": mate(o)}, device_id_type=MESH))

    loads = [pltpu.make_async_copy(src, dst, small_sem.at[n]) for n, (src, dst) in enumerate([
        (kc_in, kc), (rc_in, rc), (deg_in, deg), (vec_in, vec), (ener_in, ener), (kq_in, kq), (om_in, om), (ph_in, ph)])]
    for c in loads[:3]:
        c.start()
    load = pltpu.make_async_copy(coup, xbuf, xsem)
    load.start()
    for c in loads[3:]:
        c.start()
    for c in loads[:3]:
        c.wait()

    kpad = jnp.concatenate(
        [kc[...].astype(F32), jnp.zeros((5, ka), F32)], axis=0)
    if ka < LANES:
        kpad = jnp.concatenate([kpad, jnp.zeros((8, LANES - ka), F32)], axis=1)
    kcol = jnp.transpose(jnp.concatenate([kpad, jnp.zeros((LANES - 8, LANES), F32)], axis=0))[:ka]
    rrow = rc[...].astype(F32)
    turns = (kcol[:, 0:1] * rrow[0:1, :] + kcol[:, 1:2] * rrow[1:2, :]) + kcol[:, 2:3] * rrow[2:3, :]
    x = turns - 64.0 * jnp.floor(turns * (1.0 / 64.0))
    quad = jnp.floor((x + 8.0) * (1.0 / 16.0))
    a = (x - 16.0 * quad) * (2.0 * math.pi / 64.0)
    a2 = a * a
    sin_a = a + a * a2 * (-1.0 / 6 + a2 * (1.0 / 120 + a2 * (-1.0 / 5040 + a2 * (1.0 / 362880))))
    cos_a = 1.0 + a2 * (-0.5 + a2 * (1.0 / 24 + a2 * (-1.0 / 720 + a2 * (1.0 / 40320))))
    odd = (quad == 1.0) | (quad == 3.0)
    cosine = jnp.where(odd, sin_a, cos_a)
    sine = jnp.where(odd, cos_a, sin_a)
    cosine = jnp.where((quad == 1.0) | (quad == 2.0), -cosine, cosine)
    sine = jnp.where((quad == 2.0) | (quad == 3.0), -sine, sine)
    inverse = 1.0 / deg[...].reshape(1, rl).astype(F32)
    both = jnp.concatenate([cosine * inverse, sine * inverse], axis=0).astype(BF)

    load.wait()
    cut = min(256, rl)

    def product(at):
        total = jnp.dot(both[:, :cut], xbuf[:cut, at : at + 256], preferred_element_type=F32)
        if rl > cut:
            total += jnp.dot(both[:, cut:], xbuf[cut:, at : at + 256], preferred_element_type=F32)
        return total

    for j in range(4):
        re, im = product(256 * j), product(1024 + 256 * j)
        real = re[:ka] - im[ka:]
        imag = im[:ka] + re[ka:]
        for h in range(2):
            t = 2 * j + h
            sums[t * ka : (t + 1) * ka, :] = real[:, h * LANES : (h + 1) * LANES]
            sums[(8 + t) * ka : (9 + t) * ka, :] = imag[:, h * LANES : (h + 1) * LANES]

    def of_point(k):
        return sums[pl.ds(k, 16, stride=ka), :]

    def to_partner(i):
        sendc[i] = of_point(2 * i + (1 - mc)).astype(BF)
    each(ni, to_partner)

    for c in loads[3:]:
        c.wait()
    lane8 = iota((8, LANES), 1)
    v = vec[...]
    vsend[...] = v.astype(BF)
    flat[...] = jnp.zeros_like(flat)
    flat[0:1, 0:NB] = ener[...]
    erow = flat[0:8, :]
    erow = (erow + spin(erow, 32)) + (spin(erow, 64) + spin(erow, 96))
    esend[...] = erow[0:1, :]
    flat[0:1, 0:NB] = jnp.zeros((1, NB), F32)
    flat[0 : np_ * np_, 0:ql] = ph[...]
    flat[64 : 64 + np_, 0:ql] = om[...]
    posend[...] = jnp.transpose(flat[...])[:SLOTS]
    kqsend[...] = jnp.zeros_like(kqsend)
    kqsend[0:1, 0:ql] = kq[...]

    pl.semaphore_wait(barrier, ni + np_ - 1)

    def copy(src, dst, s, r, to):
        return pltpu.make_async_remote_copy(
            src_ref=src, dst_ref=dst, send_sem=s, recv_sem=r, device_id=to, device_id_type=MESH)

    def all_of(ref, count, sem):
        part = ref.at[pl.ds(0, count)]
        pltpu.make_async_copy(part, part, sem).wait()

    swap = copy(sendc, recvc, csem.at[0], csem.at[1], other)
    swap.start()

    def po_copy(o, to):
        return copy(posend, pogot.at[mp], sems.at[0], sems.at[1], {"pb": to})

    def kq_copy(o, to):
        return copy(kqsend, kqgot.at[mp], sems.at[2], sems.at[3], {"pb": to})

    def small(o):
        po_copy(o, mate(o)).start()
        kq_copy(o, mate(o)).start()
    each(np_ - 1, small)
    pogot[mp] = posend[...]
    kqgot[mp] = kqsend[...]

    nj = ni // np_

    def e_copy(o, i):
        return copy(esend, egot.at[mc * ni + mi], sems.at[4], sems.at[5], {"ka": i * 2 + mc})

    def v_slot(j):
        return vrows.at[mc * ni + mp * nj + j]

    def v_copy(j, i):
        return copy(vsend, v_slot(j), sems.at[6], sems.at[7], {"ka": i * 2 + mc})

    def z_copy(o, i):
        return copy(sendz.at[i], recvz.at[mi], sems.at[8], sems.at[9], {"ka": i * 2 + mc})

    last = mp == np_ - 1
    each(nj - 1, lambda j: v_copy(j, chip(mp + np_ * j)).start())

    @pl.when(jnp.logical_not(last))
    def _():
        v_copy(nj - 1, chip(mp + np_ * (nj - 1))).start()

    @pl.when(last)
    def _():
        vrows[mc * ni + mp * nj + nj - 1] = vsend[...]
    each(ni - 1, lambda o: e_copy(o, chip(o)).start())
    egot[mc * ni + mi] = esend[...]

    swap.wait_recv()

    def add_and_send(o):
        i = chip(o)
        sendz[i] = (of_point(2 * i + mc) + recvc[i].astype(F32)).astype(BF)
        z_copy(o, i).start()
    each(ni - 1, add_and_send)
    own = of_point(me) + recvc[mi].astype(F32)

    for blk, (s0, c0, s1, c1) in enumerate(
        [(1, 0, 1, 1), (-1, 1, 1, 0), (1, 1, -1, 0), (1, 0, 1, 1)]
    ):
        for low in range(4):
            left = s0 * spin(v[8 * c0 : 8 * c0 + 8], -32 * low)
            right = s1 * spin(v[8 * c1 : 8 * c1 + 8], 32 - 32 * low)
            val = jnp.where(lane8 < 32, left, jnp.where(lane8 < 64, right, 0.0))
            flat[pl.ds(32 * blk + low, 8, stride=4), :] = val
    table = jnp.transpose(flat[...])[:64]
    r_at, c_at = iota((64, 64), 0), iota((64, 64), 1)
    pick = (((r_at // nb) % 2) * NB + (r_at // rows) * nb + r_at % nb == c_at).astype(F32).astype(BF)
    for h, part in enumerate(pieces(table, 2)):
        fold[:, h * LANES : (h + 1) * LANES] = jnp.dot(
            pick, part, preferred_element_type=F32).astype(BF)

    q_at = iota((LANES, width), 1) // NB
    spread[...] = ((q_at // ql) * SLOTS + q_at % ql == iota((LANES, width), 0)).astype(F32).astype(BF)

    r_at, c_at = iota((512, 512), 0), iota((512, 512), 1)
    same = (r_at // LANES == (c_at // NB) % 4) & ((r_at // NB) % 4 == c_at // LANES) & (r_at % NB == c_at % NB)
    shifts[...] = same.astype(F32).astype(BF)

    all_of(pogot, np_ - 1, sems.at[1])
    all_of(kqgot, np_ - 1, sems.at[3])
    to_scalar = pltpu.make_async_copy(kqgot, kqs, ksm)
    to_scalar.start()
    got = pogot[...].reshape(np_ * SLOTS, LANES)
    if np_ * SLOTS < LANES:
        got = jnp.concatenate([got, jnp.zeros((LANES - np_ * SLOTS, LANES), F32)], axis=0)
    three = pieces(jnp.transpose(got)[:72], 3)
    three = [jnp.concatenate([p.astype(F32), jnp.zeros((8, LANES), F32)], axis=0).astype(BF) for p in three]
    for j in range(width // 256 if width % 256 == 0 else 0):
        at = slice(256 * j, 256 * j + 256)
        total = jnp.dot(three[0], spread[:, at], preferred_element_type=F32)
        total += jnp.dot(three[1], spread[:, at], preferred_element_type=F32)
        total += jnp.dot(three[2], spread[:, at], preferred_element_type=F32)
        phx[:, at] = total
    to_scalar.wait()

    @pl.when(jnp.logical_not(last))
    def _():
        all_of(vrows, nj, sems.at[7])

    @pl.when(last)
    def _():
        all_of(vrows, nj - 1, sems.at[7])

    def v_block(p, c):
        return vrows.at[pl.ds(c * ni + p * nj, nj)]

    def vp_copy(o, p, to):
        return copy(v_block(p, mc), v_block(p, mc), sems.at[10], sems.at[11], {"pb": to})
    each(np_ - 1, lambda o: vp_copy(o, mp, mate(o)).start())

    for q in range(queries):
        point = kqs[q // ql, 0, q % ql]
        c, i = lax.rem(point, 2), point // 2
        dz = lax.rem(mz - i // 2 + nz, nz) - nz // 2
        dy = lax.rem(my - lax.rem(i, 2) + 2, 2)
        o = 2 * jnp.where(dz >= 0, 2 * dz, -2 * dz - 1) + 1 - dy
        slots[0, q] = c * ni + lax.rem(o, np_) * nj + o // np_
        slots[1, q] = c * ni + i

    all_of(egot, ni - 1, sems.at[5])

    def e_half(c):
        return egot.at[pl.ds(c * ni, ni)]
    give_e = copy(e_half(mc), e_half(mc), wsem.at[2], wsem.at[3], other)
    give_e.start()
    copy(e_half(1 - mc), e_half(1 - mc), wsem.at[2], wsem.at[3], other).wait_recv()

    lane1 = iota((1, LANES), 1) // NB
    row_e = iota((rows, LANES), 0) % nb + mp * nb
    e_col = jnp.sum(
        jnp.where(iota((rows, LANES), 1) == row_e, esend[...], 0.0), axis=1, keepdims=True)

    def occupations(t):
        at = pl.ds(pl.multiple_of(t * LANES, LANES), LANES)
        e4 = [egot[slots[1, 4 * t + g]] for g in range(4)]
        e_there = jnp.where(lane1 < 2, jnp.where(lane1 == 0, e4[0], e4[1]), jnp.where(lane1 == 2, e4[2], e4[3]))
        fermi = 1.0 / (1.0 + jnp.exp(e_there * (1.0 / THERMAL)))
        gap = e_col - e_there
        omega = phx[64 : 64 + np_, at]
        bose = 1.0 / (jnp.exp(omega * (1.0 / THERMAL)) - 1.0)
        scale = SMEARING / (math.pi * queries)
        for m in range(np_):
            w, b = omega[m : m + 1], bose[m : m + 1]
            up, down = gap + w, gap - w
            value = (b + fermi) * (scale / (up * up + SMEARING * SMEARING))
            value += (b + 1.0 - fermi) * (scale / (down * down + SMEARING * SMEARING))
            occ[m, :, at] = value
    each(tiles, occupations, unroll=2)

    all_of(recvz, ni - 1, sems.at[9])
    terms = [own] + [recvz[chip(o)].astype(F32) for o in range(ni - 1)]
    while len(terms) > 1:
        terms = [terms[n] + terms[n + 1] for n in range(0, len(terms) - 1, 2)] + terms[len(terms) & ~1 :]
    wann = terms[0].astype(BF).astype(F32)
    blocks = []
    for low in range(4):
        for part in range(2):
            at = 64 * part
            w0 = spin(wann[0:8], at - 32 * low)
            w1 = spin(wann[8:16], at + 32 - 32 * low)
            blocks.append(jnp.where(
                (lane8 >= at) & (lane8 < at + 32), w0,
                jnp.where((lane8 >= at + 32) & (lane8 < at + 64), w1, 0.0)))
    right = jnp.concatenate(blocks + [jnp.zeros((64, LANES), F32)], axis=0).astype(BF)
    right = jnp.concatenate([right, right], axis=1)
    folded = lax.dot_general(
        fold[...], right, (((1,), (1,)), ((), ())), preferred_element_type=F32)
    for p in range(np_):
        fsend[p] = folded[p * rows : (p + 1) * rows]

    def f_copy(o, to):
        return copy(fsend.at[to], fgot.at[mp], sems.at[12], sems.at[13], {"pb": to})
    each(np_ - 1, lambda o: f_copy(o, mate(o)).start())
    fgot[mp] = fsend[mp]

    all_of(vrows, (np_ - 1) * nj, sems.at[11])

    def v_half(c):
        return vrows.at[pl.ds(c * ni, ni)]
    give_v = copy(v_half(mc), v_half(mc), wsem.at[0], wsem.at[1], other)
    give_v.start()

    swap.wait_send()
    give_e.wait_send()

    all_of(sendz, ni - 1, sems.at[8])
    all_of(egot, ni - 1, sems.at[4])

    @pl.when(jnp.logical_not(last))
    def _():
        all_of(vrows, nj, sems.at[6])

    @pl.when(last)
    def _():
        all_of(vrows, nj - 1, sems.at[6])
    all_of(pogot, np_ - 1, sems.at[0])
    all_of(kqgot, np_ - 1, sems.at[2])
    all_of(vrows, (np_ - 1) * nj, sems.at[10])

    copy(v_half(1 - mc), v_half(1 - mc), wsem.at[0], wsem.at[1], other).wait_recv()

    def take(t):
        for g in range(4):
            raw[pl.ds(pl.multiple_of(t * 16, 16), 16), g * LANES : (g + 1) * LANES] = vrows[slots[0, 4 * t + g]]
    each(tiles, take, unroll=4)
    for h in range(2):
        moved = jnp.dot(raw[...], shifts[:, 256 * h : 256 * h + 256], preferred_element_type=F32).astype(BF)
        for low in range(2):
            for t in range(tiles):
                vq[32 * h + 16 * low : 32 * h + 16 * low + 16, t * LANES : (t + 1) * LANES] = moved[
                    16 * t : 16 * t + 16, low * LANES : (low + 1) * LANES]

    all_of(fgot, np_ - 1, sems.at[13])
    left = fgot[...].reshape(np_ * rows, LANES)[:, :64].astype(BF)

    def finish(t, total):
        at = pl.ds(pl.multiple_of(t * 256, 256), 256)
        h = jnp.dot(left, vq[:, at], preferred_element_type=F32)
        for m in range(np_):
            g = phx[m : m + 1, at] * h[0:rows]
            for w in range(1, np_):
                g += phx[w * np_ + m : w * np_ + m + 1, at] * h[w * rows : (w + 1) * rows]
            total += (g * g) * occ[m, :, at]
        return total
    total = lax.fori_loop(0, width // 256, finish, jnp.zeros((rows, 256), F32), unroll=True)
    summed = jnp.sum(total, axis=1, keepdims=True)
    out[...] = jnp.sum(
        jnp.where(iota((rows, LANES), 1) == iota((rows, LANES), 0) % nb, summed, 0.0),
        axis=0, keepdims=True)[:, :nb]

    give_v.wait_send()
    all_of(fgot, np_ - 1, sems.at[12])


def shards(mesh, coupling, eigvec, energies, k_coords, r_coords, degeneracy, kq_index, omega, phonon_modes):
    np_, ka = mesh.shape["pb"], mesh.shape["ka"]
    rl = coupling.shape[0]
    ql = omega.shape[0]
    ni = ka // 2
    nb = NB // np_
    rows = 2 * nb
    width = ql * np_ * NB
    vm = pl.BlockSpec(memory_space=pltpu.VMEM)
    hbm = pl.BlockSpec(memory_space=pl.ANY)
    V = pltpu.VMEM
    sem = pltpu.SemaphoreType.DMA
    return pl.pallas_call(
        functools.partial(body, np_, ka, ql),
        out_shape=jax.ShapeDtypeStruct((1, nb), F32),
        in_specs=[hbm] * 9,
        out_specs=vm,
        scratch_shapes=[
            V((16, LANES), F32),
            V((1, NB), F32),
            V((3, ka), jnp.int32),
            V((3, rl), jnp.int32),
            V((rl,), jnp.int32),
            V((1, ql), jnp.int32),
            V((np_, ql), F32),
            V((np_ * np_, ql), F32),
            V((rl, 2048), BF),
            V((16 * ka, LANES), F32),
            V((ni, 16, LANES), BF),
            V((ni, 16, LANES), BF),
            V((ni, 16, LANES), BF),
            V((ni, 16, LANES), BF),
            V((16, LANES), BF),
            V((2 * ni, 16, LANES), BF),
            V((1, LANES), F32),
            V((2 * ni, 1, LANES), F32),
            V((LANES, LANES), F32),
            V((SLOTS, LANES), F32),
            V((np_, SLOTS, LANES), F32),
            V((1, LANES), jnp.int32),
            V((np_, 1, LANES), jnp.int32),
            pltpu.SMEM((np_, 1, LANES), jnp.int32),
            V((LANES, width), BF),
            V((80, width), F32),
            V((64, 256), BF),
            V((np_, rows, LANES), F32),
            V((np_, rows, LANES), F32),
            pltpu.SMEM((2, ql * np_), jnp.int32),
            V((512, 512), BF),
            V((width // 8, 512), BF),
            V((64, width), BF),
            V((np_, rows, width), F32),
            sem((8,)),
            sem, sem((2,)), sem((4,)), sem, sem((14,)),
        ],
        compiler_params=pltpu.CompilerParams(collective_id=0, has_side_effects=True),
        name="self_energy",
    )(
        coupling.reshape(rl, 2048),
        eigvec.reshape(16, LANES),
        energies,
        k_coords,
        r_coords,
        degeneracy,
        kq_index,
        omega.T,
        jnp.transpose(phonon_modes, (1, 2, 0)).reshape(np_ * np_, ql),
    )


def solution(mesh):
    in_specs = (
        P("ka", "pb", None),
        P("ka", None),
        P("ka", None),
        P(),
        P(None, "ka"),
        P("ka"),
        P("ka", "pb"),
        P("pb", None),
        P("pb", None, None),
    )
    return jax.shard_map(
        functools.partial(shards, mesh), mesh=mesh, in_specs=in_specs,
        out_specs=P("ka", "pb"), check_vma=False)
```

```python
import functools
import math

import jax
import jax.numpy as jnp
from jax import lax
from jax.experimental import pallas as pl
from jax.experimental.pallas import tpu as pltpu
from jax.sharding import PartitionSpec as P

THERMAL = 0.1
SMEARING = 0.05
NB = 32
LANES = 128
SLOTS = 16
MESH = pl.DeviceIdType.MESH
BF = jnp.bfloat16
F32 = jnp.float32


def iota(shape, dim):
    return lax.broadcasted_iota(jnp.int32, shape, dim)


def spin(x, shift):
    shift = shift % LANES
    return x if shift == 0 else pltpu.roll(x, shift, 1)


def pieces(x, count):
    out = []
    for _ in range(count):
        part = x.astype(BF)
        out.append(part)
        x = x - part.astype(F32)
    return out


def body(
    np_, ka, ql,
    coup, vec_in, ener_in, kc_in, rc_in, deg_in, kq_in, om_in, ph_in,
    out,
    vec, ener, kc, rc, deg, kq, om, ph,
    xbuf, sums, sendc, recvc, sendz, recvz, vsend, vrows, esend, egot,
    flat, posend, pogot, kqsend, kqgot, kqs, spread, phx, fold, fsend, fgot,
    slots, shifts, raw, vq, occ, small_sem,
    xsem, csem, wsem, ksm, sems,
):
    ni = ka // 2
    nz = ni // 2
    nb = NB // np_
    rows = 2 * nb
    queries = ql * np_
    width = queries * NB
    tiles = width // LANES
    rl = coup.shape[0]
    me = lax.axis_index("ka")
    mp = lax.axis_index("pb")
    mc = lax.rem(me, 2)
    mi = me // 2
    mz = mi // 2
    my = lax.rem(mi, 2)
    other = {"ka": mi * 2 + (1 - mc)}

    def chip(o):
        s = o // 2
        dz = nz // 2 + ((s + 1) // 2) * (1 - 2 * lax.rem(s, 2))
        z = lax.rem(mz + dz + nz, nz)
        y = lax.rem(my + 1 - lax.rem(o, 2), 2)
        return z * 2 + y

    def mate(o):
        return lax.rem(mp + 1 + o, np_)

    def each(count, f, unroll=True):
        def step(o, carry):
            f(o)
            return carry
        if count:
            lax.fori_loop(0, count, step, 0, unroll=unroll)

    barrier = pltpu.get_barrier_semaphore()
    each(ni - 1, lambda o: pl.semaphore_signal(
        barrier, inc=1, device_id={"ka": chip(o) * 2 + mc}, device_id_type=MESH))
    pl.semaphore_signal(barrier, inc=1, device_id=other, device_id_type=MESH)
    each(np_ - 1, lambda o: pl.semaphore_signal(
        barrier, inc=1, device_id={"pb": mate(o)}, device_id_type=MESH))

    loads = [pltpu.make_async_copy(src, dst, small_sem.at[n]) for n, (src, dst) in enumerate([
        (kc_in, kc), (rc_in, rc), (deg_in, deg), (vec_in, vec), (ener_in, ener), (kq_in, kq), (om_in, om), (ph_in, ph)])]
    for c in loads[:3]:
        c.start()
    load = pltpu.make_async_copy(coup, xbuf, xsem)
    load.start()
    for c in loads[3:]:
        c.start()
    for c in loads[:3]:
        c.wait()

    kpad = jnp.concatenate(
        [kc[...].astype(F32), jnp.zeros((5, ka), F32)], axis=0)
    if ka < LANES:
        kpad = jnp.concatenate([kpad, jnp.zeros((8, LANES - ka), F32)], axis=1)
    kcol = jnp.transpose(jnp.concatenate([kpad, jnp.zeros((LANES - 8, LANES), F32)], axis=0))[:ka]
    rrow = rc[...].astype(F32)
    turns = (kcol[:, 0:1] * rrow[0:1, :] + kcol[:, 1:2] * rrow[1:2, :]) + kcol[:, 2:3] * rrow[2:3, :]
    x = turns - 64.0 * jnp.floor(turns * (1.0 / 64.0))
    quad = jnp.floor((x + 8.0) * (1.0 / 16.0))
    a = (x - 16.0 * quad) * (2.0 * math.pi / 64.0)
    a2 = a * a
    sin_a = a + a * a2 * (-1.0 / 6 + a2 * (1.0 / 120 + a2 * (-1.0 / 5040 + a2 * (1.0 / 362880))))
    cos_a = 1.0 + a2 * (-0.5 + a2 * (1.0 / 24 + a2 * (-1.0 / 720 + a2 * (1.0 / 40320))))
    odd = (quad == 1.0) | (quad == 3.0)
    cosine = jnp.where(odd, sin_a, cos_a)
    sine = jnp.where(odd, cos_a, sin_a)
    cosine = jnp.where((quad == 1.0) | (quad == 2.0), -cosine, cosine)
    sine = jnp.where((quad == 2.0) | (quad == 3.0), -sine, sine)
    inverse = 1.0 / deg[...].reshape(1, rl).astype(F32)
    both = jnp.concatenate([cosine * inverse, sine * inverse], axis=0).astype(BF)

    load.wait()
    cut = min(256, rl)

    def product(at):
        total = jnp.dot(both[:, :cut], xbuf[:cut, at : at + 256], preferred_element_type=F32)
        if rl > cut:
            total += jnp.dot(both[:, cut:], xbuf[cut:, at : at + 256], preferred_element_type=F32)
        return total

    for j in range(4):
        re, im = product(256 * j), product(1024 + 256 * j)
        real = re[:ka] - im[ka:]
        imag = im[:ka] + re[ka:]
        for h in range(2):
            t = 2 * j + h
            sums[t * ka : (t + 1) * ka, :] = real[:, h * LANES : (h + 1) * LANES]
            sums[(8 + t) * ka : (9 + t) * ka, :] = imag[:, h * LANES : (h + 1) * LANES]

    def of_point(k):
        return sums[pl.ds(k, 16, stride=ka), :]

    def to_partner(i):
        sendc[i] = of_point(2 * i + (1 - mc)).astype(BF)
    each(ni, to_partner)

    for c in loads[3:]:
        c.wait()
    lane8 = iota((8, LANES), 1)
    v = vec[...]
    vsend[...] = v.astype(BF)
    flat[...] = jnp.zeros_like(flat)
    flat[0:1, 0:NB] = ener[...]
    erow = flat[0:8, :]
    erow = (erow + spin(erow, 32)) + (spin(erow, 64) + spin(erow, 96))
    esend[...] = erow[0:1, :]
    flat[0:1, 0:NB] = jnp.zeros((1, NB), F32)
    flat[0 : np_ * np_, 0:ql] = ph[...]
    flat[64 : 64 + np_, 0:ql] = om[...]
    posend[...] = jnp.transpose(flat[...])[:SLOTS]
    kqsend[...] = jnp.zeros_like(kqsend)
    kqsend[0:1, 0:ql] = kq[...]

    pl.semaphore_wait(barrier, ni + np_ - 1)

    def copy(src, dst, s, r, to):
        return pltpu.make_async_remote_copy(
            src_ref=src, dst_ref=dst, send_sem=s, recv_sem=r, device_id=to, device_id_type=MESH)

    def all_of(ref, count, sem):
        part = ref.at[pl.ds(0, count)]
        pltpu.make_async_copy(part, part, sem).wait()

    swap = copy(sendc, recvc, csem.at[0], csem.at[1], other)
    swap.start()

    def po_copy(o, to):
        return copy(posend, pogot.at[mp], sems.at[0], sems.at[1], {"pb": to})

    def kq_copy(o, to):
        return copy(kqsend, kqgot.at[mp], sems.at[2], sems.at[3], {"pb": to})

    def small(o):
        po_copy(o, mate(o)).start()
        kq_copy(o, mate(o)).start()
    each(np_ - 1, small)
    pogot[mp] = posend[...]
    kqgot[mp] = kqsend[...]

    nj = ni // np_

    def e_copy(o, i):
        return copy(esend, egot.at[mc * ni + mi], sems.at[4], sems.at[5], {"ka": i * 2 + mc})

    def v_slot(j):
        return vrows.at[mc * ni + mp * nj + j]

    def v_copy(j, i):
        return copy(vsend, v_slot(j), sems.at[6], sems.at[7], {"ka": i * 2 + mc})

    def z_copy(o, i):
        return copy(sendz.at[i], recvz.at[mi], sems.at[8], sems.at[9], {"ka": i * 2 + mc})

    last = mp == np_ - 1
    each(nj - 1, lambda j: v_copy(j, chip(mp + np_ * j)).start())

    @pl.when(jnp.logical_not(last))
    def _():
        v_copy(nj - 1, chip(mp + np_ * (nj - 1))).start()

    @pl.when(last)
    def _():
        vrows[mc * ni + mp * nj + nj - 1] = vsend[...]
    each(ni - 1, lambda o: e_copy(o, chip(o)).start())
    egot[mc * ni + mi] = esend[...]

    swap.wait_recv()

    def add_and_send(o):
        i = chip(o)
        sendz[i] = (of_point(2 * i + mc) + recvc[i].astype(F32)).astype(BF)
        z_copy(o, i).start()
    each(ni - 1, add_and_send)
    own = of_point(me) + recvc[mi].astype(F32)

    for blk, (s0, c0, s1, c1) in enumerate(
        [(1, 0, 1, 1), (-1, 1, 1, 0), (1, 1, -1, 0), (1, 0, 1, 1)]
    ):
        for low in range(4):
            left = s0 * spin(v[8 * c0 : 8 * c0 + 8], -32 * low)
            right = s1 * spin(v[8 * c1 : 8 * c1 + 8], 32 - 32 * low)
            val = jnp.where(lane8 < 32, left, jnp.where(lane8 < 64, right, 0.0))
            flat[pl.ds(32 * blk + low, 8, stride=4), :] = val
    table = jnp.transpose(flat[...])[:64]
    r_at, c_at = iota((64, 64), 0), iota((64, 64), 1)
    pick = (((r_at // nb) % 2) * NB + (r_at // rows) * nb + r_at % nb == c_at).astype(F32).astype(BF)
    for h, part in enumerate(pieces(table, 2)):
        fold[:, h * LANES : (h + 1) * LANES] = jnp.dot(
            pick, part, preferred_element_type=F32).astype(BF)

    q_at = iota((LANES, width), 1) // NB
    spread[...] = ((q_at // ql) * SLOTS + q_at % ql == iota((LANES, width), 0)).astype(F32).astype(BF)

    r_at, c_at = iota((512, 512), 0), iota((512, 512), 1)
    same = (r_at // LANES == (c_at // NB) % 4) & ((r_at // NB) % 4 == c_at // LANES) & (r_at % NB == c_at % NB)
    shifts[...] = same.astype(F32).astype(BF)

    all_of(pogot, np_ - 1, sems.at[1])
    all_of(kqgot, np_ - 1, sems.at[3])
    to_scalar = pltpu.make_async_copy(kqgot, kqs, ksm)
    to_scalar.start()
    got = pogot[...].reshape(np_ * SLOTS, LANES)
    if np_ * SLOTS < LANES:
        got = jnp.concatenate([got, jnp.zeros((LANES - np_ * SLOTS, LANES), F32)], axis=0)
    three = pieces(jnp.transpose(got)[:72], 3)
    three = [jnp.concatenate([p.astype(F32), jnp.zeros((8, LANES), F32)], axis=0).astype(BF) for p in three]
    for j in range(width // 256 if width % 256 == 0 else 0):
        at = slice(256 * j, 256 * j + 256)
        total = jnp.dot(three[0], spread[:, at], preferred_element_type=F32)
        total += jnp.dot(three[1], spread[:, at], preferred_element_type=F32)
        total += jnp.dot(three[2], spread[:, at], preferred_element_type=F32)
        phx[:, at] = total
    to_scalar.wait()

    @pl.when(jnp.logical_not(last))
    def _():
        all_of(vrows, nj, sems.at[7])

    @pl.when(last)
    def _():
        all_of(vrows, nj - 1, sems.at[7])

    def v_block(p, c):
        return vrows.at[pl.ds(c * ni + p * nj, nj)]

    def vp_copy(o, p, to):
        return copy(v_block(p, mc), v_block(p, mc), sems.at[10], sems.at[11], {"pb": to})
    each(np_ - 1, lambda o: vp_copy(o, mp, mate(o)).start())

    for q in range(queries):
        point = kqs[q // ql, 0, q % ql]
        c, i = lax.rem(point, 2), point // 2
        dz = lax.rem(mz - i // 2 + nz, nz) - nz // 2
        dy = lax.rem(my - lax.rem(i, 2) + 2, 2)
        o = 2 * jnp.where(dz >= 0, 2 * dz, -2 * dz - 1) + 1 - dy
        slots[0, q] = c * ni + lax.rem(o, np_) * nj + o // np_
        slots[1, q] = c * ni + i

    all_of(egot, ni - 1, sems.at[5])

    def e_half(c):
        return egot.at[pl.ds(c * ni, ni)]
    give_e = copy(e_half(mc), e_half(mc), wsem.at[2], wsem.at[3], other)
    give_e.start()
    copy(e_half(1 - mc), e_half(1 - mc), wsem.at[2], wsem.at[3], other).wait_recv()

    lane1 = iota((1, LANES), 1) // NB
    row_e = iota((rows, LANES), 0) % nb + mp * nb
    e_col = jnp.sum(
        jnp.where(iota((rows, LANES), 1) == row_e, esend[...], 0.0), axis=1, keepdims=True)

    def occupations(t):
        at = pl.ds(pl.multiple_of(t * LANES, LANES), LANES)
        e4 = [egot[slots[1, 4 * t + g]] for g in range(4)]
        e_there = jnp.where(lane1 < 2, jnp.where(lane1 == 0, e4[0], e4[1]), jnp.where(lane1 == 2, e4[2], e4[3]))
        fermi = 1.0 / (1.0 + jnp.exp(e_there * (1.0 / THERMAL)))
        gap = e_col - e_there
        omega = phx[64 : 64 + np_, at]
        bose = 1.0 / (jnp.exp(omega * (1.0 / THERMAL)) - 1.0)
        scale = SMEARING / (math.pi * queries)
        for m in range(np_):
            w, b = omega[m : m + 1], bose[m : m + 1]
            up, down = gap + w, gap - w
            value = (b + fermi) * (scale / (up * up + SMEARING * SMEARING))
            value += (b + 1.0 - fermi) * (scale / (down * down + SMEARING * SMEARING))
            occ[m, :, at] = value
    each(tiles, occupations, unroll=2)

    all_of(recvz, ni - 1, sems.at[9])
    terms = [own] + [recvz[chip(o)].astype(F32) for o in range(ni - 1)]
    while len(terms) > 1:
        terms = [terms[n] + terms[n + 1] for n in range(0, len(terms) - 1, 2)] + terms[len(terms) & ~1 :]
    wann = terms[0].astype(BF).astype(F32)
    blocks = []
    for low in range(4):
        for part in range(2):
            at = 64 * part
            w0 = spin(wann[0:8], at - 32 * low)
            w1 = spin(wann[8:16], at + 32 - 32 * low)
            blocks.append(jnp.where(
                (lane8 >= at) & (lane8 < at + 32), w0,
                jnp.where((lane8 >= at + 32) & (lane8 < at + 64), w1, 0.0)))
    right = jnp.concatenate(blocks + [jnp.zeros((64, LANES), F32)], axis=0).astype(BF)
    right = jnp.concatenate([right, right], axis=1)
    folded = lax.dot_general(
        fold[...], right, (((1,), (1,)), ((), ())), preferred_element_type=F32)
    for p in range(np_):
        fsend[p] = folded[p * rows : (p + 1) * rows]

    def f_copy(o, to):
        return copy(fsend.at[to], fgot.at[mp], sems.at[12], sems.at[13], {"pb": to})
    each(np_ - 1, lambda o: f_copy(o, mate(o)).start())
    fgot[mp] = fsend[mp]

    all_of(vrows, (np_ - 1) * nj, sems.at[11])

    def v_half(c):
        return vrows.at[pl.ds(c * ni, ni)]
    give_v = copy(v_half(mc), v_half(mc), wsem.at[0], wsem.at[1], other)
    give_v.start()

    swap.wait_send()
    give_e.wait_send()

    all_of(sendz, ni - 1, sems.at[8])
    all_of(egot, ni - 1, sems.at[4])

    @pl.when(jnp.logical_not(last))
    def _():
        all_of(vrows, nj, sems.at[6])

    @pl.when(last)
    def _():
        all_of(vrows, nj - 1, sems.at[6])
    all_of(pogot, np_ - 1, sems.at[0])
    all_of(kqgot, np_ - 1, sems.at[2])
    all_of(vrows, (np_ - 1) * nj, sems.at[10])

    copy(v_half(1 - mc), v_half(1 - mc), wsem.at[0], wsem.at[1], other).wait_recv()

    def take(t):
        for g in range(4):
            raw[pl.ds(pl.multiple_of(t * 16, 16), 16), g * LANES : (g + 1) * LANES] = vrows[slots[0, 4 * t + g]]
    each(tiles, take, unroll=4)
    for h in range(2):
        moved = jnp.dot(raw[...], shifts[:, 256 * h : 256 * h + 256], preferred_element_type=F32).astype(BF)
        for low in range(2):
            for t in range(tiles):
                vq[32 * h + 16 * low : 32 * h + 16 * low + 16, t * LANES : (t + 1) * LANES] = moved[
                    16 * t : 16 * t + 16, low * LANES : (low + 1) * LANES]

    all_of(fgot, np_ - 1, sems.at[13])
    left = fgot[...].reshape(np_ * rows, LANES)[:, :64].astype(BF)

    def finish(t, total):
        at = pl.ds(pl.multiple_of(t * 256, 256), 256)
        h = jnp.dot(left, vq[:, at], preferred_element_type=F32)
        for m in range(np_):
            g = phx[m : m + 1, at] * h[0:rows]
            for w in range(1, np_):
                g += phx[w * np_ + m : w * np_ + m + 1, at] * h[w * rows : (w + 1) * rows]
            total += (g * g) * occ[m, :, at]
        return total
    total = lax.fori_loop(0, width // 256, finish, jnp.zeros((rows, 256), F32), unroll=True)
    summed = jnp.sum(total, axis=1, keepdims=True)
    out[...] = jnp.sum(
        jnp.where(iota((rows, LANES), 1) == iota((rows, LANES), 0) % nb, summed, 0.0),
        axis=0, keepdims=True)[:, :nb]

    give_v.wait_send()
    all_of(fgot, np_ - 1, sems.at[12])


def shards(mesh, coupling, eigvec, energies, k_coords, r_coords, degeneracy, kq_index, omega, phonon_modes):
    np_, ka = mesh.shape["pb"], mesh.shape["ka"]
    rl = coupling.shape[0]
    ql = omega.shape[0]
    ni = ka // 2
    nb = NB // np_
    rows = 2 * nb
    width = ql * np_ * NB
    vm = pl.BlockSpec(memory_space=pltpu.VMEM)
    hbm = pl.BlockSpec(memory_space=pl.ANY)
    V = pltpu.VMEM
    sem = pltpu.SemaphoreType.DMA
    return pl.pallas_call(
        functools.partial(body, np_, ka, ql),
        out_shape=pltpu.VMEM((1, nb), F32),
        in_specs=[hbm] * 9,
        out_specs=vm,
        scratch_shapes=[
            V((16, LANES), F32),
            V((1, NB), F32),
            V((3, ka), jnp.int32),
            V((3, rl), jnp.int32),
            V((rl,), jnp.int32),
            V((1, ql), jnp.int32),
            V((np_, ql), F32),
            V((np_ * np_, ql), F32),
            V((rl, 2048), BF),
            V((16 * ka, LANES), F32),
            V((ni, 16, LANES), BF),
            V((ni, 16, LANES), BF),
            V((ni, 16, LANES), BF),
            V((ni, 16, LANES), BF),
            V((16, LANES), BF),
            V((2 * ni, 16, LANES), BF),
            V((1, LANES), F32),
            V((2 * ni, 1, LANES), F32),
            V((LANES, LANES), F32),
            V((SLOTS, LANES), F32),
            V((np_, SLOTS, LANES), F32),
            V((1, LANES), jnp.int32),
            V((np_, 1, LANES), jnp.int32),
            pltpu.SMEM((np_, 1, LANES), jnp.int32),
            V((LANES, width), BF),
            V((80, width), F32),
            V((64, 256), BF),
            V((np_, rows, LANES), F32),
            V((np_, rows, LANES), F32),
            pltpu.SMEM((2, ql * np_), jnp.int32),
            V((512, 512), BF),
            V((width // 8, 512), BF),
            V((64, width), BF),
            V((np_, rows, width), F32),
            sem((8,)),
            sem, sem((2,)), sem((4,)), sem, sem((14,)),
        ],
        compiler_params=pltpu.CompilerParams(collective_id=0, has_side_effects=True),
        name="self_energy",
    )(
        coupling.reshape(rl, 2048),
        eigvec.reshape(16, LANES),
        energies,
        k_coords,
        r_coords,
        degeneracy,
        kq_index,
        omega.T,
        jnp.transpose(phonon_modes, (1, 2, 0)).reshape(np_ * np_, ql),
    )


def solution(mesh):
    in_specs = (
        P("ka", "pb", None),
        P("ka", None),
        P("ka", None),
        P(),
        P(None, "ka"),
        P("ka"),
        P("ka", "pb"),
        P("pb", None),
        P("pb", None, None),
    )
    return jax.shard_map(
        functools.partial(shards, mesh), mesh=mesh, in_specs=in_specs,
        out_specs=P("ka", "pb"), check_vma=False)
```

```python
import functools
import math

import jax
import jax.numpy as jnp
from jax import lax
from jax.experimental import pallas as pl
from jax.experimental.pallas import tpu as pltpu
from jax.sharding import PartitionSpec as P

THERMAL = 0.1
SMEARING = 0.05
NB = 32
LANES = 128
SLOTS = 16
MESH = pl.DeviceIdType.MESH
BF = jnp.bfloat16
F32 = jnp.float32


def iota(shape, dim):
    return lax.broadcasted_iota(jnp.int32, shape, dim)


def spin(x, shift):
    shift = shift % LANES
    return x if shift == 0 else pltpu.roll(x, shift, 1)


def pieces(x, count):
    out = []
    for _ in range(count):
        part = x.astype(BF)
        out.append(part)
        x = x - part.astype(F32)
    return out


def body(
    np_, ka, ql,
    coup, vec_in, ener_in, kc_in, rc_in, deg_in, kq_in, om_in, ph_in,
    out,
    vec, ener, kc, rc, deg, kq, om, ph,
    xbuf, sums, sendc, recvc, sendz, recvz, vsend, vrows, esend, egot,
    flat, posend, pogot, kqsend, kqgot, kqs, spread, phx, fold, fsend, fgot,
    slots, shifts, raw, vq, occ, small_sem,
    xsem, csem, wsem, ksm, sems,
):
    ni = ka // 2
    nz = ni // 2
    nb = NB // np_
    rows = 2 * nb
    queries = ql * np_
    width = queries * NB
    tiles = width // LANES
    rl = coup.shape[0]
    me = lax.axis_index("ka")
    mp = lax.axis_index("pb")
    mc = lax.rem(me, 2)
    mi = me // 2
    mz = mi // 2
    my = lax.rem(mi, 2)
    other = {"ka": mi * 2 + (1 - mc)}

    def chip(o):
        s = o // 2
        dz = nz // 2 + ((s + 1) // 2) * (1 - 2 * lax.rem(s, 2))
        z = lax.rem(mz + dz + nz, nz)
        y = lax.rem(my + 1 - lax.rem(o, 2), 2)
        return z * 2 + y

    def in_z_order(f):
        for z in range(nz):
            f(z * 2 + 1 - my)

            @pl.when(mz != z)
            def _():
                f(z * 2 + my)

    def mate(o):
        return lax.rem(mp + 1 + o, np_)

    def each(count, f, unroll=True):
        def step(o, carry):
            f(o)
            return carry
        if count:
            lax.fori_loop(0, count, step, 0, unroll=unroll)

    barrier = pltpu.get_barrier_semaphore()
    each(ni - 1, lambda o: pl.semaphore_signal(
        barrier, inc=1, device_id={"ka": chip(o) * 2 + mc}, device_id_type=MESH))
    pl.semaphore_signal(barrier, inc=1, device_id=other, device_id_type=MESH)
    each(np_ - 1, lambda o: pl.semaphore_signal(
        barrier, inc=1, device_id={"pb": mate(o)}, device_id_type=MESH))

    loads = [pltpu.make_async_copy(src, dst, small_sem.at[n]) for n, (src, dst) in enumerate([
        (kc_in, kc), (rc_in, rc), (deg_in, deg), (vec_in, vec), (ener_in, ener), (kq_in, kq), (om_in, om), (ph_in, ph)])]
    for c in loads[:3]:
        c.start()
    load = pltpu.make_async_copy(coup, xbuf, xsem)
    load.start()
    for c in loads[3:]:
        c.start()
    for c in loads[:3]:
        c.wait()

    kpad = jnp.concatenate(
        [kc[...].astype(F32), jnp.zeros((5, ka), F32)], axis=0)
    if ka < LANES:
        kpad = jnp.concatenate([kpad, jnp.zeros((8, LANES - ka), F32)], axis=1)
    kcol = jnp.transpose(jnp.concatenate([kpad, jnp.zeros((LANES - 8, LANES), F32)], axis=0))[:ka]
    rrow = rc[...].astype(F32)
    turns = (kcol[:, 0:1] * rrow[0:1, :] + kcol[:, 1:2] * rrow[1:2, :]) + kcol[:, 2:3] * rrow[2:3, :]
    x = turns - 64.0 * jnp.floor(turns * (1.0 / 64.0))
    quad = jnp.floor((x + 8.0) * (1.0 / 16.0))
    a = (x - 16.0 * quad) * (2.0 * math.pi / 64.0)
    a2 = a * a
    sin_a = a + a * a2 * (-1.0 / 6 + a2 * (1.0 / 120 + a2 * (-1.0 / 5040 + a2 * (1.0 / 362880))))
    cos_a = 1.0 + a2 * (-0.5 + a2 * (1.0 / 24 + a2 * (-1.0 / 720 + a2 * (1.0 / 40320))))
    odd = (quad == 1.0) | (quad == 3.0)
    cosine = jnp.where(odd, sin_a, cos_a)
    sine = jnp.where(odd, cos_a, sin_a)
    cosine = jnp.where((quad == 1.0) | (quad == 2.0), -cosine, cosine)
    sine = jnp.where((quad == 2.0) | (quad == 3.0), -sine, sine)
    inverse = 1.0 / deg[...].reshape(1, rl).astype(F32)
    both = jnp.concatenate([cosine * inverse, sine * inverse], axis=0).astype(BF)

    load.wait()
    cut = min(256, rl)

    def product(at):
        total = jnp.dot(both[:, :cut], xbuf[:cut, at : at + 256], preferred_element_type=F32)
        if rl > cut:
            total += jnp.dot(both[:, cut:], xbuf[cut:, at : at + 256], preferred_element_type=F32)
        return total

    for j in range(4):
        re, im = product(256 * j), product(1024 + 256 * j)
        real = re[:ka] - im[ka:]
        imag = im[:ka] + re[ka:]
        for h in range(2):
            t = 2 * j + h
            sums[t * ka : (t + 1) * ka, :] = real[:, h * LANES : (h + 1) * LANES]
            sums[(8 + t) * ka : (9 + t) * ka, :] = imag[:, h * LANES : (h + 1) * LANES]

    def of_point(k):
        return sums[pl.ds(k, 16, stride=ka), :]

    def to_partner(i):
        sendc[i] = of_point(2 * i + (1 - mc)).astype(BF)
    each(ni, to_partner)

    for c in loads[3:]:
        c.wait()
    lane8 = iota((8, LANES), 1)
    v = vec[...]
    vsend[...] = v.astype(BF)
    flat[...] = jnp.zeros_like(flat)
    flat[0:1, 0:NB] = ener[...]
    erow = flat[0:8, :]
    erow = (erow + spin(erow, 32)) + (spin(erow, 64) + spin(erow, 96))
    esend[...] = erow[0:1, :]
    flat[0:1, 0:NB] = jnp.zeros((1, NB), F32)
    flat[0 : np_ * np_, 0:ql] = ph[...]
    flat[64 : 64 + np_, 0:ql] = om[...]
    posend[...] = jnp.transpose(flat[...])[:SLOTS]
    kqsend[...] = jnp.zeros_like(kqsend)
    kqsend[0:1, 0:ql] = kq[...]

    pl.semaphore_wait(barrier, ni + np_ - 1)

    def copy(src, dst, s, r, to):
        return pltpu.make_async_remote_copy(
            src_ref=src, dst_ref=dst, send_sem=s, recv_sem=r, device_id=to, device_id_type=MESH)

    def all_of(ref, count, sem):
        part = ref.at[pl.ds(0, count)]
        pltpu.make_async_copy(part, part, sem).wait()

    swap = copy(sendc, recvc, csem.at[0], csem.at[1], other)
    swap.start()

    def po_copy(o, to):
        return copy(posend, pogot.at[mp], sems.at[0], sems.at[1], {"pb": to})

    def kq_copy(o, to):
        return copy(kqsend, kqgot.at[mp], sems.at[2], sems.at[3], {"pb": to})

    def small(o):
        po_copy(o, mate(o)).start()
        kq_copy(o, mate(o)).start()
    each(np_ - 1, small)
    pogot[mp] = posend[...]
    kqgot[mp] = kqsend[...]

    nj = ni // np_

    def e_copy(o, i):
        return copy(esend, egot.at[mc * ni + mi], sems.at[4], sems.at[5], {"ka": i * 2 + mc})

    def v_slot(j):
        return vrows.at[mc * ni + mp * nj + j]

    def v_copy(j, i):
        return copy(vsend, v_slot(j), sems.at[6], sems.at[7], {"ka": i * 2 + mc})

    def z_copy(o, i):
        return copy(sendz.at[i], recvz.at[mi], sems.at[8], sems.at[9], {"ka": i * 2 + mc})

    last = mp == np_ - 1
    each(nj - 1, lambda j: v_copy(j, chip(mp + np_ * j)).start())

    @pl.when(jnp.logical_not(last))
    def _():
        v_copy(nj - 1, chip(mp + np_ * (nj - 1))).start()

    @pl.when(last)
    def _():
        vrows[mc * ni + mp * nj + nj - 1] = vsend[...]
    in_z_order(lambda i: e_copy(0, i).start())
    egot[mc * ni + mi] = esend[...]

    swap.wait_recv()

    def add_and_send(i):
        sendz[i] = (of_point(2 * i + mc) + recvc[i].astype(F32)).astype(BF)
        z_copy(0, i).start()
    in_z_order(add_and_send)
    own = of_point(me) + recvc[mi].astype(F32)

    for blk, (s0, c0, s1, c1) in enumerate(
        [(1, 0, 1, 1), (-1, 1, 1, 0), (1, 1, -1, 0), (1, 0, 1, 1)]
    ):
        for low in range(4):
            left = s0 * spin(v[8 * c0 : 8 * c0 + 8], -32 * low)
            right = s1 * spin(v[8 * c1 : 8 * c1 + 8], 32 - 32 * low)
            val = jnp.where(lane8 < 32, left, jnp.where(lane8 < 64, right, 0.0))
            flat[pl.ds(32 * blk + low, 8, stride=4), :] = val
    table = jnp.transpose(flat[...])[:64]
    r_at, c_at = iota((64, 64), 0), iota((64, 64), 1)
    pick = (((r_at // nb) % 2) * NB + (r_at // rows) * nb + r_at % nb == c_at).astype(F32).astype(BF)
    for h, part in enumerate(pieces(table, 2)):
        fold[:, h * LANES : (h + 1) * LANES] = jnp.dot(
            pick, part, preferred_element_type=F32).astype(BF)

    q_at = iota((LANES, width), 1) // NB
    spread[...] = ((q_at // ql) * SLOTS + q_at % ql == iota((LANES, width), 0)).astype(F32).astype(BF)

    r_at, c_at = iota((512, 512), 0), iota((512, 512), 1)
    same = (r_at // LANES == (c_at // NB) % 4) & ((r_at // NB) % 4 == c_at // LANES) & (r_at % NB == c_at % NB)
    shifts[...] = same.astype(F32).astype(BF)

    all_of(pogot, np_ - 1, sems.at[1])
    all_of(kqgot, np_ - 1, sems.at[3])
    to_scalar = pltpu.make_async_copy(kqgot, kqs, ksm)
    to_scalar.start()
    got = pogot[...].reshape(np_ * SLOTS, LANES)
    if np_ * SLOTS < LANES:
        got = jnp.concatenate([got, jnp.zeros((LANES - np_ * SLOTS, LANES), F32)], axis=0)
    three = pieces(jnp.transpose(got)[:72], 3)
    three = [jnp.concatenate([p.astype(F32), jnp.zeros((8, LANES), F32)], axis=0).astype(BF) for p in three]
    for j in range(width // 256 if width % 256 == 0 else 0):
        at = slice(256 * j, 256 * j + 256)
        total = jnp.dot(three[0], spread[:, at], preferred_element_type=F32)
        total += jnp.dot(three[1], spread[:, at], preferred_element_type=F32)
        total += jnp.dot(three[2], spread[:, at], preferred_element_type=F32)
        phx[:, at] = total
    to_scalar.wait()

    @pl.when(jnp.logical_not(last))
    def _():
        all_of(vrows, nj, sems.at[7])

    @pl.when(last)
    def _():
        all_of(vrows, nj - 1, sems.at[7])

    def v_block(p, c):
        return vrows.at[pl.ds(c * ni + p * nj, nj)]

    def vp_copy(o, p, to):
        return copy(v_block(p, mc), v_block(p, mc), sems.at[10], sems.at[11], {"pb": to})
    each(np_ - 1, lambda o: vp_copy(o, mp, mate(o)).start())

    for q in range(queries):
        point = kqs[q // ql, 0, q % ql]
        c, i = lax.rem(point, 2), point // 2
        dz = lax.rem(mz - i // 2 + nz, nz) - nz // 2
        dy = lax.rem(my - lax.rem(i, 2) + 2, 2)
        o = 2 * jnp.where(dz >= 0, 2 * dz, -2 * dz - 1) + 1 - dy
        slots[0, q] = c * ni + lax.rem(o, np_) * nj + o // np_
        slots[1, q] = c * ni + i

    all_of(egot, ni - 1, sems.at[5])

    def e_half(c):
        return egot.at[pl.ds(c * ni, ni)]
    give_e = copy(e_half(mc), e_half(mc), wsem.at[2], wsem.at[3], other)
    give_e.start()

    all_of(recvz, ni - 1, sems.at[9])
    terms = [own] + [recvz[chip(o)].astype(F32) for o in range(ni - 1)]
    while len(terms) > 1:
        terms = [terms[n] + terms[n + 1] for n in range(0, len(terms) - 1, 2)] + terms[len(terms) & ~1 :]
    wann = terms[0].astype(BF).astype(F32)
    blocks = []
    for low in range(4):
        for part in range(2):
            at = 64 * part
            w0 = spin(wann[0:8], at - 32 * low)
            w1 = spin(wann[8:16], at + 32 - 32 * low)
            blocks.append(jnp.where(
                (lane8 >= at) & (lane8 < at + 32), w0,
                jnp.where((lane8 >= at + 32) & (lane8 < at + 64), w1, 0.0)))
    right = jnp.concatenate(blocks + [jnp.zeros((64, LANES), F32)], axis=0).astype(BF)
    right = jnp.concatenate([right, right], axis=1)
    folded = lax.dot_general(
        fold[...], right, (((1,), (1,)), ((), ())), preferred_element_type=F32)
    for p in range(np_):
        fsend[p] = folded[p * rows : (p + 1) * rows]

    def f_copy(o, to):
        return copy(fsend.at[to], fgot.at[mp], sems.at[12], sems.at[13], {"pb": to})
    each(np_ - 1, lambda o: f_copy(o, mate(o)).start())
    fgot[mp] = fsend[mp]

    all_of(vrows, (np_ - 1) * nj, sems.at[11])

    def v_half(c):
        return vrows.at[pl.ds(c * ni, ni)]
    give_v = copy(v_half(mc), v_half(mc), wsem.at[0], wsem.at[1], other)
    give_v.start()

    copy(e_half(1 - mc), e_half(1 - mc), wsem.at[2], wsem.at[3], other).wait_recv()

    lane1 = iota((1, LANES), 1) // NB
    row_e = iota((rows, LANES), 0) % nb + mp * nb
    e_col = jnp.sum(
        jnp.where(iota((rows, LANES), 1) == row_e, esend[...], 0.0), axis=1, keepdims=True)

    def occupations(t):
        at = pl.ds(pl.multiple_of(t * LANES, LANES), LANES)
        e4 = [egot[slots[1, 4 * t + g]] for g in range(4)]
        e_there = jnp.where(lane1 < 2, jnp.where(lane1 == 0, e4[0], e4[1]), jnp.where(lane1 == 2, e4[2], e4[3]))
        fermi = 1.0 / (1.0 + jnp.exp(e_there * (1.0 / THERMAL)))
        gap = e_col - e_there
        omega = phx[64 : 64 + np_, at]
        bose = 1.0 / (jnp.exp(omega * (1.0 / THERMAL)) - 1.0)
        scale = SMEARING / (math.pi * queries)
        for m in range(np_):
            w, b = omega[m : m + 1], bose[m : m + 1]
            up, down = gap + w, gap - w
            value = (b + fermi) * (scale / (up * up + SMEARING * SMEARING))
            value += (b + 1.0 - fermi) * (scale / (down * down + SMEARING * SMEARING))
            occ[m, :, at] = value
    each(tiles, occupations, unroll=2)


    swap.wait_send()
    give_e.wait_send()

    all_of(sendz, ni - 1, sems.at[8])
    all_of(egot, ni - 1, sems.at[4])

    @pl.when(jnp.logical_not(last))
    def _():
        all_of(vrows, nj, sems.at[6])

    @pl.when(last)
    def _():
        all_of(vrows, nj - 1, sems.at[6])
    all_of(pogot, np_ - 1, sems.at[0])
    all_of(kqgot, np_ - 1, sems.at[2])
    all_of(vrows, (np_ - 1) * nj, sems.at[10])

    copy(v_half(1 - mc), v_half(1 - mc), wsem.at[0], wsem.at[1], other).wait_recv()

    def take(t):
        for g in range(4):
            raw[pl.ds(pl.multiple_of(t * 16, 16), 16), g * LANES : (g + 1) * LANES] = vrows[slots[0, 4 * t + g]]
    each(tiles, take, unroll=4)
    for h in range(2):
        moved = jnp.dot(raw[...], shifts[:, 256 * h : 256 * h + 256], preferred_element_type=F32).astype(BF)
        for low in range(2):
            for t in range(tiles):
                vq[32 * h + 16 * low : 32 * h + 16 * low + 16, t * LANES : (t + 1) * LANES] = moved[
                    16 * t : 16 * t + 16, low * LANES : (low + 1) * LANES]

    all_of(fgot, np_ - 1, sems.at[13])
    left = fgot[...].reshape(np_ * rows, LANES)[:, :64].astype(BF)

    def finish(t, total):
        at = pl.ds(pl.multiple_of(t * 256, 256), 256)
        h = jnp.dot(left, vq[:, at], preferred_element_type=F32)
        for m in range(np_):
            g = phx[m : m + 1, at] * h[0:rows]
            for w in range(1, np_):
                g += phx[w * np_ + m : w * np_ + m + 1, at] * h[w * rows : (w + 1) * rows]
            total += (g * g) * occ[m, :, at]
        return total
    total = lax.fori_loop(0, width // 256, finish, jnp.zeros((rows, 256), F32), unroll=True)
    summed = jnp.sum(total, axis=1, keepdims=True)
    out[...] = jnp.sum(
        jnp.where(iota((rows, LANES), 1) == iota((rows, LANES), 0) % nb, summed, 0.0),
        axis=0, keepdims=True)[:, :nb]

    give_v.wait_send()
    all_of(fgot, np_ - 1, sems.at[12])


def shards(mesh, coupling, eigvec, energies, k_coords, r_coords, degeneracy, kq_index, omega, phonon_modes):
    np_, ka = mesh.shape["pb"], mesh.shape["ka"]
    rl = coupling.shape[0]
    ql = omega.shape[0]
    ni = ka // 2
    nb = NB // np_
    rows = 2 * nb
    width = ql * np_ * NB
    vm = pl.BlockSpec(memory_space=pltpu.VMEM)
    hbm = pl.BlockSpec(memory_space=pl.ANY)
    V = pltpu.VMEM
    sem = pltpu.SemaphoreType.DMA
    return pl.pallas_call(
        functools.partial(body, np_, ka, ql),
        out_shape=pltpu.VMEM((1, nb), F32),
        in_specs=[hbm] * 9,
        out_specs=vm,
        scratch_shapes=[
            V((16, LANES), F32),
            V((1, NB), F32),
            V((3, ka), jnp.int32),
            V((3, rl), jnp.int32),
            V((rl,), jnp.int32),
            V((1, ql), jnp.int32),
            V((np_, ql), F32),
            V((np_ * np_, ql), F32),
            V((rl, 2048), BF),
            V((16 * ka, LANES), F32),
            V((ni, 16, LANES), BF),
            V((ni, 16, LANES), BF),
            V((ni, 16, LANES), BF),
            V((ni, 16, LANES), BF),
            V((16, LANES), BF),
            V((2 * ni, 16, LANES), BF),
            V((1, LANES), F32),
            V((2 * ni, 1, LANES), F32),
            V((LANES, LANES), F32),
            V((SLOTS, LANES), F32),
            V((np_, SLOTS, LANES), F32),
            V((1, LANES), jnp.int32),
            V((np_, 1, LANES), jnp.int32),
            pltpu.SMEM((np_, 1, LANES), jnp.int32),
            V((LANES, width), BF),
            V((80, width), F32),
            V((64, 256), BF),
            V((np_, rows, LANES), F32),
            V((np_, rows, LANES), F32),
            pltpu.SMEM((2, ql * np_), jnp.int32),
            V((512, 512), BF),
            V((width // 8, 512), BF),
            V((64, width), BF),
            V((np_, rows, width), F32),
            sem((8,)),
            sem, sem((2,)), sem((4,)), sem, sem((14,)),
        ],
        compiler_params=pltpu.CompilerParams(collective_id=0, has_side_effects=True),
        name="self_energy",
    )(
        coupling.reshape(rl, 2048),
        eigvec.reshape(16, LANES),
        energies,
        k_coords,
        r_coords,
        degeneracy,
        kq_index,
        omega.T,
        jnp.transpose(phonon_modes, (1, 2, 0)).reshape(np_ * np_, ql),
    )


def solution(mesh):
    in_specs = (
        P("ka", "pb", None),
        P("ka", None),
        P("ka", None),
        P(),
        P(None, "ka"),
        P("ka"),
        P("ka", "pb"),
        P("pb", None),
        P("pb", None, None),
    )
    return jax.shard_map(
        functools.partial(shards, mesh), mesh=mesh, in_specs=in_specs,
        out_specs=P("ka", "pb"), check_vma=False)
```

```python
import functools
import math

import jax
import jax.numpy as jnp
from jax import lax
from jax.experimental import pallas as pl
from jax.experimental.pallas import tpu as pltpu
from jax.sharding import PartitionSpec as P

THERMAL = 0.1
SMEARING = 0.05
NB = 32
LANES = 128
SLOTS = 16
MESH = pl.DeviceIdType.MESH
BF = jnp.bfloat16
F32 = jnp.float32


def iota(shape, dim):
    return lax.broadcasted_iota(jnp.int32, shape, dim)


def spin(x, shift):
    shift = shift % LANES
    return x if shift == 0 else pltpu.roll(x, shift, 1)


def pieces(x, count):
    out = []
    for _ in range(count):
        part = x.astype(BF)
        out.append(part)
        x = x - part.astype(F32)
    return out


def body(
    np_, ka, ql,
    coup, vec_in, ener_in, kc_in, rc_in, deg_in, kq_in, om_in, ph_in,
    out,
    vec, ener, kc, rc, deg, kq, om, ph,
    xbuf, sums, sendc, recvc, sendz, recvz, vsend, vrows, esend, egot,
    flat, posend, pogot, kqsend, kqgot, kqs, spread, phx, fold, fsend, fgot,
    slots, shifts, raw, vq, occ, small_sem,
    xsem, csem, wsem, ksm, sems,
):
    ni = ka // 2
    nz = ni // 2
    nb = NB // np_
    rows = 2 * nb
    queries = ql * np_
    width = queries * NB
    tiles = width // LANES
    rl = coup.shape[0]
    me = lax.axis_index("ka")
    mp = lax.axis_index("pb")
    mc = lax.rem(me, 2)
    mi = me // 2
    mz = mi // 2
    my = lax.rem(mi, 2)
    other = {"ka": mi * 2 + (1 - mc)}

    def chip(o):
        s = o // 2
        dz = nz // 2 + ((s + 1) // 2) * (1 - 2 * lax.rem(s, 2))
        z = lax.rem(mz + dz + nz, nz)
        y = lax.rem(my + 1 - lax.rem(o, 2), 2)
        return z * 2 + y

    def in_z_order(f, before={}):
        for z in range(nz):
            if z in before:
                before[z]()
            f(z * 2 + 1 - my)

            @pl.when(mz != z)
            def _():
                f(z * 2 + my)

    def mate(o):
        return lax.rem(mp + 1 + o, np_)

    def each(count, f, unroll=True):
        def step(o, carry):
            f(o)
            return carry
        if count:
            lax.fori_loop(0, count, step, 0, unroll=unroll)

    barrier = pltpu.get_barrier_semaphore()
    each(ni - 1, lambda o: pl.semaphore_signal(
        barrier, inc=1, device_id={"ka": chip(o) * 2 + mc}, device_id_type=MESH))
    pl.semaphore_signal(barrier, inc=1, device_id=other, device_id_type=MESH)
    each(np_ - 1, lambda o: pl.semaphore_signal(
        barrier, inc=1, device_id={"pb": mate(o)}, device_id_type=MESH))
    each(np_ - 1, lambda o: pl.semaphore_signal(
        barrier, inc=1, device_id={"pb": mate(o), **other}, device_id_type=MESH))

    loads = [pltpu.make_async_copy(src, dst, small_sem.at[n]) for n, (src, dst) in enumerate([
        (kc_in, kc), (rc_in, rc), (deg_in, deg), (vec_in, vec), (ener_in, ener), (kq_in, kq), (om_in, om), (ph_in, ph)])]
    for c in loads[:3]:
        c.start()
    load = pltpu.make_async_copy(coup, xbuf, xsem)
    load.start()
    for c in loads[3:]:
        c.start()
    for c in loads[:3]:
        c.wait()

    kpad = jnp.concatenate(
        [kc[...].astype(F32), jnp.zeros((5, ka), F32)], axis=0)
    if ka < LANES:
        kpad = jnp.concatenate([kpad, jnp.zeros((8, LANES - ka), F32)], axis=1)
    kcol = jnp.transpose(jnp.concatenate([kpad, jnp.zeros((LANES - 8, LANES), F32)], axis=0))[:ka]
    rrow = rc[...].astype(F32)
    turns = (kcol[:, 0:1] * rrow[0:1, :] + kcol[:, 1:2] * rrow[1:2, :]) + kcol[:, 2:3] * rrow[2:3, :]
    x = turns - 64.0 * jnp.floor(turns * (1.0 / 64.0))
    quad = jnp.floor((x + 8.0) * (1.0 / 16.0))
    a = (x - 16.0 * quad) * (2.0 * math.pi / 64.0)
    a2 = a * a
    sin_a = a + a * a2 * (-1.0 / 6 + a2 * (1.0 / 120 + a2 * (-1.0 / 5040 + a2 * (1.0 / 362880))))
    cos_a = 1.0 + a2 * (-0.5 + a2 * (1.0 / 24 + a2 * (-1.0 / 720 + a2 * (1.0 / 40320))))
    odd = (quad == 1.0) | (quad == 3.0)
    cosine = jnp.where(odd, sin_a, cos_a)
    sine = jnp.where(odd, cos_a, sin_a)
    cosine = jnp.where((quad == 1.0) | (quad == 2.0), -cosine, cosine)
    sine = jnp.where((quad == 2.0) | (quad == 3.0), -sine, sine)
    inverse = 1.0 / deg[...].reshape(1, rl).astype(F32)
    both = jnp.concatenate([cosine * inverse, sine * inverse], axis=0).astype(BF)

    load.wait()
    cut = min(256, rl)

    def product(at):
        total = jnp.dot(both[:, :cut], xbuf[:cut, at : at + 256], preferred_element_type=F32)
        if rl > cut:
            total += jnp.dot(both[:, cut:], xbuf[cut:, at : at + 256], preferred_element_type=F32)
        return total

    for j in range(4):
        re, im = product(256 * j), product(1024 + 256 * j)
        real = re[:ka] - im[ka:]
        imag = im[:ka] + re[ka:]
        for h in range(2):
            t = 2 * j + h
            sums[t * ka : (t + 1) * ka, :] = real[:, h * LANES : (h + 1) * LANES]
            sums[(8 + t) * ka : (9 + t) * ka, :] = imag[:, h * LANES : (h + 1) * LANES]

    def of_point(k):
        return sums[pl.ds(k, 16, stride=ka), :]

    def to_partner(i):
        sendc[i] = of_point(2 * i + (1 - mc)).astype(BF)
    each(ni, to_partner)

    for c in loads[3:]:
        c.wait()
    lane8 = iota((8, LANES), 1)
    v = vec[...]
    vsend[...] = v.astype(BF)
    flat[...] = jnp.zeros_like(flat)
    flat[0:1, 0:NB] = ener[...]
    erow = flat[0:8, :]
    erow = (erow + spin(erow, 32)) + (spin(erow, 64) + spin(erow, 96))
    esend[...] = erow[0:1, :]
    flat[0:1, 0:NB] = jnp.zeros((1, NB), F32)
    flat[0 : np_ * np_, 0:ql] = ph[...]
    flat[64 : 64 + np_, 0:ql] = om[...]
    posend[...] = jnp.transpose(flat[...])[:SLOTS]
    kqsend[...] = jnp.zeros_like(kqsend)
    kqsend[0:1, 0:ql] = kq[...]

    pl.semaphore_wait(barrier, ni + 2 * (np_ - 1))

    def copy(src, dst, s, r, to):
        return pltpu.make_async_remote_copy(
            src_ref=src, dst_ref=dst, send_sem=s, recv_sem=r, device_id=to, device_id_type=MESH)

    def all_of(ref, count, sem):
        part = ref.at[pl.ds(0, count)]
        pltpu.make_async_copy(part, part, sem).wait()

    cut_at = 8
    swap = copy(sendc.at[pl.ds(0, cut_at)], recvc.at[pl.ds(0, cut_at)], csem.at[0], csem.at[1], other)
    swap_rest = copy(
        sendc.at[pl.ds(cut_at, ni - cut_at)], recvc.at[pl.ds(cut_at, ni - cut_at)], wsem.at[0], wsem.at[1], other)
    swap.start()
    swap_rest.start()

    def po_copy(o, to):
        return copy(posend, pogot.at[mp], sems.at[0], sems.at[1], {"pb": to})

    def kq_copy(o, to):
        return copy(kqsend, kqgot.at[mp], sems.at[2], sems.at[3], {"pb": to})

    def small(o):
        po_copy(o, mate(o)).start()
        kq_copy(o, mate(o)).start()
    each(np_ - 1, small)
    pogot[mp] = posend[...]
    kqgot[mp] = kqsend[...]

    nj = ni // np_

    def e_copy(o, i):
        return copy(esend, egot.at[mc * ni + mi], sems.at[4], sems.at[5], {"ka": i * 2 + mc})

    def v_slot(j):
        return vrows.at[mc * ni + mp * nj + j]

    def v_copy(j, i):
        return copy(vsend, v_slot(j), sems.at[6], sems.at[7], {"ka": i * 2 + mc})

    def z_copy(o, i):
        return copy(sendz.at[i], recvz.at[mi], sems.at[8], sems.at[9], {"ka": i * 2 + mc})

    last = mp == np_ - 1
    each(nj - 1, lambda j: v_copy(j, chip(mp + np_ * j)).start())

    @pl.when(jnp.logical_not(last))
    def _():
        v_copy(nj - 1, chip(mp + np_ * (nj - 1))).start()

    @pl.when(last)
    def _():
        vrows[mc * ni + mp * nj + nj - 1] = vsend[...]
    in_z_order(lambda i: e_copy(0, i).start())
    egot[mc * ni + mi] = esend[...]

    swap.wait_recv()

    def add_and_send(i):
        sendz[i] = (of_point(2 * i + mc) + recvc[i].astype(F32)).astype(BF)
        z_copy(0, i).start()
    in_z_order(add_and_send, {cut_at // 2: swap_rest.wait_recv})
    own = of_point(me) + recvc[mi].astype(F32)

    for blk, (s0, c0, s1, c1) in enumerate(
        [(1, 0, 1, 1), (-1, 1, 1, 0), (1, 1, -1, 0), (1, 0, 1, 1)]
    ):
        for low in range(4):
            left = s0 * spin(v[8 * c0 : 8 * c0 + 8], -32 * low)
            right = s1 * spin(v[8 * c1 : 8 * c1 + 8], 32 - 32 * low)
            val = jnp.where(lane8 < 32, left, jnp.where(lane8 < 64, right, 0.0))
            flat[pl.ds(32 * blk + low, 8, stride=4), :] = val
    table = jnp.transpose(flat[...])[:64]
    r_at, c_at = iota((64, 64), 0), iota((64, 64), 1)
    pick = (((r_at // nb) % 2) * NB + (r_at // rows) * nb + r_at % nb == c_at).astype(F32).astype(BF)
    for h, part in enumerate(pieces(table, 2)):
        fold[:, h * LANES : (h + 1) * LANES] = jnp.dot(
            pick, part, preferred_element_type=F32).astype(BF)

    q_at = iota((LANES, width), 1) // NB
    spread[...] = ((q_at // ql) * SLOTS + q_at % ql == iota((LANES, width), 0)).astype(F32).astype(BF)

    r_at, c_at = iota((512, 512), 0), iota((512, 512), 1)
    same = (r_at // LANES == (c_at // NB) % 4) & ((r_at // NB) % 4 == c_at // LANES) & (r_at % NB == c_at % NB)
    shifts[...] = same.astype(F32).astype(BF)

    all_of(pogot, np_ - 1, sems.at[1])
    all_of(kqgot, np_ - 1, sems.at[3])
    to_scalar = pltpu.make_async_copy(kqgot, kqs, ksm)
    to_scalar.start()
    got = pogot[...].reshape(np_ * SLOTS, LANES)
    if np_ * SLOTS < LANES:
        got = jnp.concatenate([got, jnp.zeros((LANES - np_ * SLOTS, LANES), F32)], axis=0)
    three = pieces(jnp.transpose(got)[:72], 3)
    three = [jnp.concatenate([p.astype(F32), jnp.zeros((8, LANES), F32)], axis=0).astype(BF) for p in three]
    for j in range(width // 256 if width % 256 == 0 else 0):
        at = slice(256 * j, 256 * j + 256)
        total = jnp.dot(three[0], spread[:, at], preferred_element_type=F32)
        total += jnp.dot(three[1], spread[:, at], preferred_element_type=F32)
        total += jnp.dot(three[2], spread[:, at], preferred_element_type=F32)
        phx[:, at] = total
    to_scalar.wait()

    @pl.when(jnp.logical_not(last))
    def _():
        all_of(vrows, nj, sems.at[7])

    @pl.when(last)
    def _():
        all_of(vrows, nj - 1, sems.at[7])

    def v_block(p, c):
        return vrows.at[pl.ds(c * ni + p * nj, nj)]

    def vp_copy(o, p, to):
        return copy(v_block(p, mc), v_block(p, mc), sems.at[10], sems.at[11], {"pb": to})

    def to_other_core(to):
        return copy(v_block(mp, mc), v_block(mp, mc), sems.at[10], sems.at[11], {**to, **other})

    def spread_v(o):
        vp_copy(o, mp, mate(o)).start()
        to_other_core({"pb": mate(o)}).start()
    each(np_ - 1, spread_v)
    to_other_core({}).start()

    for q in range(queries):
        point = kqs[q // ql, 0, q % ql]
        c, i = lax.rem(point, 2), point // 2
        dz = lax.rem(mz - i // 2 + nz, nz) - nz // 2
        dy = lax.rem(my - lax.rem(i, 2) + 2, 2)
        o = 2 * jnp.where(dz >= 0, 2 * dz, -2 * dz - 1) + 1 - dy
        slots[0, q] = c * ni + lax.rem(o, np_) * nj + o // np_
        slots[1, q] = c * ni + i

    all_of(egot, ni - 1, sems.at[5])

    def e_half(c):
        return egot.at[pl.ds(c * ni, ni)]
    give_e = copy(e_half(mc), e_half(mc), wsem.at[2], wsem.at[3], other)
    give_e.start()

    all_of(recvz, ni - 1, sems.at[9])
    terms = [own] + [recvz[chip(o)].astype(F32) for o in range(ni - 1)]
    while len(terms) > 1:
        terms = [terms[n] + terms[n + 1] for n in range(0, len(terms) - 1, 2)] + terms[len(terms) & ~1 :]
    wann = terms[0].astype(BF).astype(F32)
    blocks = []
    for low in range(4):
        for part in range(2):
            at = 64 * part
            w0 = spin(wann[0:8], at - 32 * low)
            w1 = spin(wann[8:16], at + 32 - 32 * low)
            blocks.append(jnp.where(
                (lane8 >= at) & (lane8 < at + 32), w0,
                jnp.where((lane8 >= at + 32) & (lane8 < at + 64), w1, 0.0)))
    right = jnp.concatenate(blocks + [jnp.zeros((64, LANES), F32)], axis=0).astype(BF)
    right = jnp.concatenate([right, right], axis=1)
    folded = lax.dot_general(
        fold[...], right, (((1,), (1,)), ((), ())), preferred_element_type=F32)
    for p in range(np_):
        fsend[p] = folded[p * rows : (p + 1) * rows]

    def f_copy(o, to):
        return copy(fsend.at[to], fgot.at[mp], sems.at[12], sems.at[13], {"pb": to})
    each(np_ - 1, lambda o: f_copy(o, mate(o)).start())
    fgot[mp] = fsend[mp]

    copy(e_half(1 - mc), e_half(1 - mc), wsem.at[2], wsem.at[3], other).wait_recv()

    lane1 = iota((1, LANES), 1) // NB
    row_e = iota((rows, LANES), 0) % nb + mp * nb
    e_col = jnp.sum(
        jnp.where(iota((rows, LANES), 1) == row_e, esend[...], 0.0), axis=1, keepdims=True)

    def occupations(t):
        at = pl.ds(pl.multiple_of(t * LANES, LANES), LANES)
        e4 = [egot[slots[1, 4 * t + g]] for g in range(4)]
        e_there = jnp.where(lane1 < 2, jnp.where(lane1 == 0, e4[0], e4[1]), jnp.where(lane1 == 2, e4[2], e4[3]))
        fermi = 1.0 / (1.0 + jnp.exp(e_there * (1.0 / THERMAL)))
        gap = e_col - e_there
        omega = phx[64 : 64 + np_, at]
        bose = 1.0 / (jnp.exp(omega * (1.0 / THERMAL)) - 1.0)
        scale = SMEARING / (math.pi * queries)
        for m in range(np_):
            w, b = omega[m : m + 1], bose[m : m + 1]
            up, down = gap + w, gap - w
            value = (b + fermi) * (scale / (up * up + SMEARING * SMEARING))
            value += (b + 1.0 - fermi) * (scale / (down * down + SMEARING * SMEARING))
            occ[m, :, at] = value
    each(tiles, occupations, unroll=2)


    all_of(vrows, (2 * np_ - 1) * nj, sems.at[11])

    swap.wait_send()
    swap_rest.wait_send()
    give_e.wait_send()

    all_of(sendz, ni - 1, sems.at[8])
    all_of(egot, ni - 1, sems.at[4])

    @pl.when(jnp.logical_not(last))
    def _():
        all_of(vrows, nj, sems.at[6])

    @pl.when(last)
    def _():
        all_of(vrows, nj - 1, sems.at[6])
    all_of(pogot, np_ - 1, sems.at[0])
    all_of(kqgot, np_ - 1, sems.at[2])
    all_of(vrows, (2 * np_ - 1) * nj, sems.at[10])

    def take(t):
        for g in range(4):
            raw[pl.ds(pl.multiple_of(t * 16, 16), 16), g * LANES : (g + 1) * LANES] = vrows[slots[0, 4 * t + g]]
    each(tiles, take, unroll=4)
    for h in range(2):
        moved = jnp.dot(raw[...], shifts[:, 256 * h : 256 * h + 256], preferred_element_type=F32).astype(BF)
        for low in range(2):
            for t in range(tiles):
                vq[32 * h + 16 * low : 32 * h + 16 * low + 16, t * LANES : (t + 1) * LANES] = moved[
                    16 * t : 16 * t + 16, low * LANES : (low + 1) * LANES]

    all_of(fgot, np_ - 1, sems.at[13])
    left = fgot[...].reshape(np_ * rows, LANES)[:, :64].astype(BF)

    def finish(t, total):
        at = pl.ds(pl.multiple_of(t * 256, 256), 256)
        h = jnp.dot(left, vq[:, at], preferred_element_type=F32)
        for m in range(np_):
            g = phx[m : m + 1, at] * h[0:rows]
            for w in range(1, np_):
                g += phx[w * np_ + m : w * np_ + m + 1, at] * h[w * rows : (w + 1) * rows]
            total += (g * g) * occ[m, :, at]
        return total
    total = lax.fori_loop(0, width // 256, finish, jnp.zeros((rows, 256), F32), unroll=True)
    summed = jnp.sum(total, axis=1, keepdims=True)
    out[...] = jnp.sum(
        jnp.where(iota((rows, LANES), 1) == iota((rows, LANES), 0) % nb, summed, 0.0),
        axis=0, keepdims=True)[:, :nb]

    all_of(fgot, np_ - 1, sems.at[12])


def shards(mesh, coupling, eigvec, energies, k_coords, r_coords, degeneracy, kq_index, omega, phonon_modes):
    np_, ka = mesh.shape["pb"], mesh.shape["ka"]
    rl = coupling.shape[0]
    ql = omega.shape[0]
    ni = ka // 2
    nb = NB // np_
    rows = 2 * nb
    width = ql * np_ * NB
    vm = pl.BlockSpec(memory_space=pltpu.VMEM)
    hbm = pl.BlockSpec(memory_space=pl.ANY)
    V = pltpu.VMEM
    sem = pltpu.SemaphoreType.DMA
    return pl.pallas_call(
        functools.partial(body, np_, ka, ql),
        out_shape=pltpu.VMEM((1, nb), F32),
        in_specs=[hbm] * 9,
        out_specs=vm,
        scratch_shapes=[
            V((16, LANES), F32),
            V((1, NB), F32),
            V((3, ka), jnp.int32),
            V((3, rl), jnp.int32),
            V((rl,), jnp.int32),
            V((1, ql), jnp.int32),
            V((np_, ql), F32),
            V((np_ * np_, ql), F32),
            V((rl, 2048), BF),
            V((16 * ka, LANES), F32),
            V((ni, 16, LANES), BF),
            V((ni, 16, LANES), BF),
            V((ni, 16, LANES), BF),
            V((ni, 16, LANES), BF),
            V((16, LANES), BF),
            V((2 * ni, 16, LANES), BF),
            V((1, LANES), F32),
            V((2 * ni, 1, LANES), F32),
            V((LANES, LANES), F32),
            V((SLOTS, LANES), F32),
            V((np_, SLOTS, LANES), F32),
            V((1, LANES), jnp.int32),
            V((np_, 1, LANES), jnp.int32),
            pltpu.SMEM((np_, 1, LANES), jnp.int32),
            V((LANES, width), BF),
            V((80, width), F32),
            V((64, 256), BF),
            V((np_, rows, LANES), F32),
            V((np_, rows, LANES), F32),
            pltpu.SMEM((2, ql * np_), jnp.int32),
            V((512, 512), BF),
            V((width // 8, 512), BF),
            V((64, width), BF),
            V((np_, rows, width), F32),
            sem((8,)),
            sem, sem((2,)), sem((4,)), sem, sem((14,)),
        ],
        compiler_params=pltpu.CompilerParams(collective_id=0, has_side_effects=True),
        name="self_energy",
    )(
        coupling.reshape(rl, 2048),
        eigvec.reshape(16, LANES),
        energies,
        k_coords,
        r_coords,
        degeneracy,
        kq_index,
        omega.T,
        jnp.transpose(phonon_modes, (1, 2, 0)).reshape(np_ * np_, ql),
    )


def solution(mesh):
    in_specs = (
        P("ka", "pb", None),
        P("ka", None),
        P("ka", None),
        P(),
        P(None, "ka"),
        P("ka"),
        P("ka", "pb"),
        P("pb", None),
        P("pb", None, None),
    )
    return jax.shard_map(
        functools.partial(shards, mesh), mesh=mesh, in_specs=in_specs,
        out_specs=P("ka", "pb"), check_vma=False)
```

```python
import functools
import math

import jax
import jax.numpy as jnp
from jax import lax
from jax.experimental import pallas as pl
from jax.experimental.pallas import tpu as pltpu
from jax.sharding import PartitionSpec as P

THERMAL = 0.1
SMEARING = 0.05
NB = 32
LANES = 128
SLOTS = 16
MESH = pl.DeviceIdType.MESH
BF = jnp.bfloat16
F32 = jnp.float32


def iota(shape, dim):
    return lax.broadcasted_iota(jnp.int32, shape, dim)


def spin(x, shift):
    shift = shift % LANES
    return x if shift == 0 else pltpu.roll(x, shift, 1)


def pieces(x, count):
    out = []
    for _ in range(count):
        part = x.astype(BF)
        out.append(part)
        x = x - part.astype(F32)
    return out


def body(
    np_, ka, ql,
    coup, vec_in, ener_in, kc_in, rc_in, deg_in, kq_in, om_in, ph_in,
    out,
    vec, ener, kc, rc, deg, kq, om, ph,
    xbuf, sums, sendc, recvc, sendz, recvz, vsend, vrows, esend, egot,
    flat, posend, pogot, kqsend, kqgot, kqs, spread, phx, fold, fsend, fgot,
    slots, shifts, raw, vq, occ,
    csem, wsem, sems,
):
    ni = ka // 2
    nz = ni // 2
    nb = NB // np_
    rows = 2 * nb
    queries = ql * np_
    width = queries * NB
    tiles = width // LANES
    rl = coup.shape[0]
    me = lax.axis_index("ka")
    mp = lax.axis_index("pb")
    mc = lax.rem(me, 2)
    mi = me // 2
    mz = mi // 2
    my = lax.rem(mi, 2)
    other = {"ka": mi * 2 + (1 - mc)}

    def chip(o):
        s = o // 2
        dz = nz // 2 + ((s + 1) // 2) * (1 - 2 * lax.rem(s, 2))
        z = lax.rem(mz + dz + nz, nz)
        y = lax.rem(my + 1 - lax.rem(o, 2), 2)
        return z * 2 + y

    def in_z_order(f):
        for z in range(nz):
            f(z * 2 + 1 - my)

            @pl.when(mz != z)
            def _():
                f(z * 2 + my)

    def mate(o):
        return lax.rem(mp + 1 + o, np_)

    def each(count, f, unroll=True):
        def step(o, carry):
            f(o)
            return carry
        if count:
            lax.fori_loop(0, count, step, 0, unroll=unroll)

    barrier = pltpu.get_barrier_semaphore()
    each(ni - 1, lambda o: pl.semaphore_signal(
        barrier, inc=1, device_id={"ka": chip(o) * 2 + mc}, device_id_type=MESH))
    pl.semaphore_signal(barrier, inc=1, device_id=other, device_id_type=MESH)
    each(np_ - 1, lambda o: pl.semaphore_signal(
        barrier, inc=1, device_id={"pb": mate(o)}, device_id_type=MESH))

    loads = [pltpu.make_async_copy(src, dst, (sems.at[2 * n] if n < 7 else csem.at[0])) for n, (src, dst) in enumerate([
        (kc_in, kc), (rc_in, rc), (deg_in, deg), (vec_in, vec), (ener_in, ener), (kq_in, kq), (om_in, om), (ph_in, ph)])]
    for c in loads[:3]:
        c.start()
    load = pltpu.make_async_copy(coup, xbuf, wsem.at[0])
    load.start()
    for c in loads[3:]:
        c.start()
    for c in loads[:3]:
        c.wait()

    kpad = jnp.concatenate(
        [kc[...].astype(F32), jnp.zeros((5, ka), F32)], axis=0)
    if ka < LANES:
        kpad = jnp.concatenate([kpad, jnp.zeros((8, LANES - ka), F32)], axis=1)
    kcol = jnp.transpose(jnp.concatenate([kpad, jnp.zeros((LANES - 8, LANES), F32)], axis=0))[:ka]
    rrow = rc[...].astype(F32)
    turns = (kcol[:, 0:1] * rrow[0:1, :] + kcol[:, 1:2] * rrow[1:2, :]) + kcol[:, 2:3] * rrow[2:3, :]
    x = turns - 64.0 * jnp.floor(turns * (1.0 / 64.0))
    quad = jnp.floor((x + 8.0) * (1.0 / 16.0))
    a = (x - 16.0 * quad) * (2.0 * math.pi / 64.0)
    a2 = a * a
    sin_a = a + a * a2 * (-1.0 / 6 + a2 * (1.0 / 120 + a2 * (-1.0 / 5040 + a2 * (1.0 / 362880))))
    cos_a = 1.0 + a2 * (-0.5 + a2 * (1.0 / 24 + a2 * (-1.0 / 720 + a2 * (1.0 / 40320))))
    odd = (quad == 1.0) | (quad == 3.0)
    cosine = jnp.where(odd, sin_a, cos_a)
    sine = jnp.where(odd, cos_a, sin_a)
    cosine = jnp.where((quad == 1.0) | (quad == 2.0), -cosine, cosine)
    sine = jnp.where((quad == 2.0) | (quad == 3.0), -sine, sine)
    inverse = 1.0 / deg[...].reshape(1, rl).astype(F32)
    both = jnp.concatenate([cosine * inverse, sine * inverse], axis=0).astype(BF)

    load.wait()
    cut = min(256, rl)

    def product(at):
        total = jnp.dot(both[:, :cut], xbuf[:cut, at : at + 256], preferred_element_type=F32)
        if rl > cut:
            total += jnp.dot(both[:, cut:], xbuf[cut:, at : at + 256], preferred_element_type=F32)
        return total

    for j in range(4):
        re, im = product(256 * j), product(1024 + 256 * j)
        real = re[:ka] - im[ka:]
        imag = im[:ka] + re[ka:]
        for h in range(2):
            t = 2 * j + h
            sums[t * ka : (t + 1) * ka, :] = real[:, h * LANES : (h + 1) * LANES]
            sums[(8 + t) * ka : (9 + t) * ka, :] = imag[:, h * LANES : (h + 1) * LANES]

    def of_point(k):
        return sums[pl.ds(k, 16, stride=ka), :]

    def to_partner(i):
        sendc[i] = of_point(2 * i + (1 - mc)).astype(BF)
    each(ni, to_partner)

    for c in loads[3:]:
        c.wait()
    lane8 = iota((8, LANES), 1)
    v = vec[...]
    vsend[...] = v.astype(BF)
    flat[...] = jnp.zeros_like(flat)
    flat[0:1, 0:NB] = ener[...]
    erow = flat[0:8, :]
    erow = (erow + spin(erow, 32)) + (spin(erow, 64) + spin(erow, 96))
    esend[...] = erow[0:1, :]
    flat[0:1, 0:NB] = jnp.zeros((1, NB), F32)
    flat[0 : np_ * np_, 0:ql] = ph[...]
    flat[64 : 64 + np_, 0:ql] = om[...]
    posend[...] = jnp.transpose(flat[...])[:SLOTS]
    kqsend[...] = jnp.zeros_like(kqsend)
    kqsend[0:1, 0:ql] = kq[...]

    pl.semaphore_wait(barrier, ni + np_ - 1)

    def copy(src, dst, s, r, to):
        return pltpu.make_async_remote_copy(
            src_ref=src, dst_ref=dst, send_sem=s, recv_sem=r, device_id=to, device_id_type=MESH)

    def all_of(ref, count, sem):
        part = ref.at[pl.ds(0, count)]
        pltpu.make_async_copy(part, part, sem).wait()

    swap = copy(sendc, recvc, csem.at[0], csem.at[1], other)
    swap.start()

    def po_copy(o, to):
        return copy(posend, pogot.at[mp], sems.at[0], sems.at[1], {"pb": to})

    def kq_copy(o, to):
        return copy(kqsend, kqgot.at[mp], sems.at[2], sems.at[3], {"pb": to})

    def small(o):
        po_copy(o, mate(o)).start()
        kq_copy(o, mate(o)).start()
    each(np_ - 1, small)
    pogot[mp] = posend[...]
    kqgot[mp] = kqsend[...]

    nj = ni // np_

    def e_copy(o, i):
        return copy(esend, egot.at[mc * ni + mi], sems.at[4], sems.at[5], {"ka": i * 2 + mc})

    def v_slot(j):
        return vrows.at[mc * ni + mp * nj + j]

    def v_copy(j, i):
        return copy(vsend, v_slot(j), sems.at[6], sems.at[7], {"ka": i * 2 + mc})

    def z_copy(o, i):
        return copy(sendz.at[i], recvz.at[mi], sems.at[8], sems.at[9], {"ka": i * 2 + mc})

    last = mp == np_ - 1
    each(nj - 1, lambda j: v_copy(j, chip(mp + np_ * j)).start())

    @pl.when(jnp.logical_not(last))
    def _():
        v_copy(nj - 1, chip(mp + np_ * (nj - 1))).start()

    @pl.when(last)
    def _():
        vrows[mc * ni + mp * nj + nj - 1] = vsend[...]
    in_z_order(lambda i: e_copy(0, i).start())
    egot[mc * ni + mi] = esend[...]

    swap.wait_recv()

    def add_and_send(i):
        sendz[i] = (of_point(2 * i + mc) + recvc[i].astype(F32)).astype(BF)
        z_copy(0, i).start()
    in_z_order(add_and_send)
    own = of_point(me) + recvc[mi].astype(F32)

    for blk, (s0, c0, s1, c1) in enumerate(
        [(1, 0, 1, 1), (-1, 1, 1, 0), (1, 1, -1, 0), (1, 0, 1, 1)]
    ):
        for low in range(4):
            left = s0 * spin(v[8 * c0 : 8 * c0 + 8], -32 * low)
            right = s1 * spin(v[8 * c1 : 8 * c1 + 8], 32 - 32 * low)
            val = jnp.where(lane8 < 32, left, jnp.where(lane8 < 64, right, 0.0))
            flat[pl.ds(32 * blk + low, 8, stride=4), :] = val
    table = jnp.transpose(flat[...])[:64]
    r_at, c_at = iota((64, 64), 0), iota((64, 64), 1)
    pick = (((r_at // nb) % 2) * NB + (r_at // rows) * nb + r_at % nb == c_at).astype(F32).astype(BF)
    for h, part in enumerate(pieces(table, 2)):
        fold[:, h * LANES : (h + 1) * LANES] = jnp.dot(
            pick, part, preferred_element_type=F32).astype(BF)

    q_at = iota((LANES, width), 1) // NB
    spread[...] = ((q_at // ql) * SLOTS + q_at % ql == iota((LANES, width), 0)).astype(F32).astype(BF)

    r_at, c_at = iota((512, 512), 0), iota((512, 512), 1)
    same = (r_at // LANES == (c_at // NB) % 4) & ((r_at // NB) % 4 == c_at // LANES) & (r_at % NB == c_at % NB)
    shifts[...] = same.astype(F32).astype(BF)

    all_of(pogot, np_ - 1, sems.at[1])
    all_of(kqgot, np_ - 1, sems.at[3])
    to_scalar = pltpu.make_async_copy(kqgot, kqs, wsem.at[0])
    to_scalar.start()
    got = pogot[...].reshape(np_ * SLOTS, LANES)
    if np_ * SLOTS < LANES:
        got = jnp.concatenate([got, jnp.zeros((LANES - np_ * SLOTS, LANES), F32)], axis=0)
    three = pieces(jnp.transpose(got)[:72], 3)
    three = [jnp.concatenate([p.astype(F32), jnp.zeros((8, LANES), F32)], axis=0).astype(BF) for p in three]
    for j in range(width // 256 if width % 256 == 0 else 0):
        at = slice(256 * j, 256 * j + 256)
        total = jnp.dot(three[0], spread[:, at], preferred_element_type=F32)
        total += jnp.dot(three[1], spread[:, at], preferred_element_type=F32)
        total += jnp.dot(three[2], spread[:, at], preferred_element_type=F32)
        phx[:, at] = total
    to_scalar.wait()

    @pl.when(jnp.logical_not(last))
    def _():
        all_of(vrows, nj, sems.at[7])

    @pl.when(last)
    def _():
        all_of(vrows, nj - 1, sems.at[7])

    def v_block(p, c):
        return vrows.at[pl.ds(c * ni + p * nj, nj)]

    def vp_copy(o, p, to):
        return copy(v_block(p, mc), v_block(p, mc), sems.at[10], sems.at[11], {"pb": to})
    each(np_ - 1, lambda o: vp_copy(o, mp, mate(o)).start())

    for q in range(queries):
        point = kqs[q // ql, 0, q % ql]
        c, i = lax.rem(point, 2), point // 2
        dz = lax.rem(mz - i // 2 + nz, nz) - nz // 2
        dy = lax.rem(my - lax.rem(i, 2) + 2, 2)
        o = 2 * jnp.where(dz >= 0, 2 * dz, -2 * dz - 1) + 1 - dy
        slots[0, q] = c * ni + lax.rem(o, np_) * nj + o // np_
        slots[1, q] = c * ni + i

    all_of(egot, ni - 1, sems.at[5])

    def e_half(c):
        return egot.at[pl.ds(c * ni, ni)]
    give_e = copy(e_half(mc), e_half(mc), wsem.at[2], wsem.at[3], other)
    give_e.start()

    all_of(recvz, ni - 1, sems.at[9])
    terms = [own] + [recvz[chip(o)].astype(F32) for o in range(ni - 1)]
    while len(terms) > 1:
        terms = [terms[n] + terms[n + 1] for n in range(0, len(terms) - 1, 2)] + terms[len(terms) & ~1 :]
    wann = terms[0].astype(BF).astype(F32)
    blocks = []
    for low in range(4):
        for part in range(2):
            at = 64 * part
            w0 = spin(wann[0:8], at - 32 * low)
            w1 = spin(wann[8:16], at + 32 - 32 * low)
            blocks.append(jnp.where(
                (lane8 >= at) & (lane8 < at + 32), w0,
                jnp.where((lane8 >= at + 32) & (lane8 < at + 64), w1, 0.0)))
    right = jnp.concatenate(blocks + [jnp.zeros((64, LANES), F32)], axis=0).astype(BF)
    right = jnp.concatenate([right, right], axis=1)
    folded = lax.dot_general(
        fold[...], right, (((1,), (1,)), ((), ())), preferred_element_type=F32)
    for p in range(np_):
        fsend[p] = folded[p * rows : (p + 1) * rows]

    def f_copy(o, to):
        return copy(fsend.at[to], fgot.at[mp], sems.at[12], sems.at[13], {"pb": to})
    each(np_ - 1, lambda o: f_copy(o, mate(o)).start())
    fgot[mp] = fsend[mp]

    all_of(vrows, (np_ - 1) * nj, sems.at[11])

    def v_half(c):
        return vrows.at[pl.ds(c * ni, ni)]
    give_v = copy(v_half(mc), v_half(mc), wsem.at[0], wsem.at[1], other)
    give_v.start()

    copy(e_half(1 - mc), e_half(1 - mc), wsem.at[2], wsem.at[3], other).wait_recv()

    lane1 = iota((1, LANES), 1) // NB
    row_e = iota((rows, LANES), 0) % nb + mp * nb
    e_col = jnp.sum(
        jnp.where(iota((rows, LANES), 1) == row_e, esend[...], 0.0), axis=1, keepdims=True)

    def occupations(t):
        at = pl.ds(pl.multiple_of(t * LANES, LANES), LANES)
        e4 = [egot[slots[1, 4 * t + g]] for g in range(4)]
        e_there = jnp.where(lane1 < 2, jnp.where(lane1 == 0, e4[0], e4[1]), jnp.where(lane1 == 2, e4[2], e4[3]))
        fermi = 1.0 / (1.0 + jnp.exp(e_there * (1.0 / THERMAL)))
        gap = e_col - e_there
        omega = phx[64 : 64 + np_, at]
        bose = 1.0 / (jnp.exp(omega * (1.0 / THERMAL)) - 1.0)
        scale = SMEARING / (math.pi * queries)
        for m in range(np_):
            w, b = omega[m : m + 1], bose[m : m + 1]
            up, down = gap + w, gap - w
            value = (b + fermi) * (scale / (up * up + SMEARING * SMEARING))
            value += (b + 1.0 - fermi) * (scale / (down * down + SMEARING * SMEARING))
            occ[m, :, at] = value
    each(tiles, occupations, unroll=2)


    swap.wait_send()
    give_e.wait_send()

    all_of(sendz, ni - 1, sems.at[8])
    all_of(egot, ni - 1, sems.at[4])

    @pl.when(jnp.logical_not(last))
    def _():
        all_of(vrows, nj, sems.at[6])

    @pl.when(last)
    def _():
        all_of(vrows, nj - 1, sems.at[6])
    all_of(pogot, np_ - 1, sems.at[0])
    all_of(kqgot, np_ - 1, sems.at[2])
    all_of(vrows, (np_ - 1) * nj, sems.at[10])

    copy(v_half(1 - mc), v_half(1 - mc), wsem.at[0], wsem.at[1], other).wait_recv()

    def take(t):
        for g in range(4):
            raw[pl.ds(pl.multiple_of(t * 16, 16), 16), g * LANES : (g + 1) * LANES] = vrows[slots[0, 4 * t + g]]
    each(tiles, take, unroll=4)
    for h in range(2):
        moved = jnp.dot(raw[...], shifts[:, 256 * h : 256 * h + 256], preferred_element_type=F32).astype(BF)
        for low in range(2):
            for t in range(tiles):
                vq[32 * h + 16 * low : 32 * h + 16 * low + 16, t * LANES : (t + 1) * LANES] = moved[
                    16 * t : 16 * t + 16, low * LANES : (low + 1) * LANES]

    all_of(fgot, np_ - 1, sems.at[13])
    left = fgot[...].reshape(np_ * rows, LANES)[:, :64].astype(BF)

    def finish(t, total):
        at = pl.ds(pl.multiple_of(t * 256, 256), 256)
        h = jnp.dot(left, vq[:, at], preferred_element_type=F32)
        for m in range(np_):
            g = phx[m : m + 1, at] * h[0:rows]
            for w in range(1, np_):
                g += phx[w * np_ + m : w * np_ + m + 1, at] * h[w * rows : (w + 1) * rows]
            total += (g * g) * occ[m, :, at]
        return total
    total = lax.fori_loop(0, width // 256, finish, jnp.zeros((rows, 256), F32), unroll=True)
    summed = jnp.sum(total, axis=1, keepdims=True)
    out[...] = jnp.sum(
        jnp.where(iota((rows, LANES), 1) == iota((rows, LANES), 0) % nb, summed, 0.0),
        axis=0, keepdims=True)[:, :nb]

    give_v.wait_send()
    all_of(fgot, np_ - 1, sems.at[12])


def shards(mesh, coupling, eigvec, energies, k_coords, r_coords, degeneracy, kq_index, omega, phonon_modes):
    np_, ka = mesh.shape["pb"], mesh.shape["ka"]
    rl = coupling.shape[0]
    ql = omega.shape[0]
    ni = ka // 2
    nb = NB // np_
    rows = 2 * nb
    width = ql * np_ * NB
    vm = pl.BlockSpec(memory_space=pltpu.VMEM)
    hbm = pl.BlockSpec(memory_space=pl.ANY)
    V = pltpu.VMEM
    sem = pltpu.SemaphoreType.DMA
    return pl.pallas_call(
        functools.partial(body, np_, ka, ql),
        out_shape=pltpu.VMEM((1, nb), F32),
        in_specs=[hbm] * 9,
        out_specs=vm,
        scratch_shapes=[
            V((16, LANES), F32),
            V((1, NB), F32),
            V((3, ka), jnp.int32),
            V((3, rl), jnp.int32),
            V((rl,), jnp.int32),
            V((1, ql), jnp.int32),
            V((np_, ql), F32),
            V((np_ * np_, ql), F32),
            V((rl, 2048), BF),
            V((16 * ka, LANES), F32),
            V((ni, 16, LANES), BF),
            V((ni, 16, LANES), BF),
            V((ni, 16, LANES), BF),
            V((ni, 16, LANES), BF),
            V((16, LANES), BF),
            V((2 * ni, 16, LANES), BF),
            V((1, LANES), F32),
            V((2 * ni, 1, LANES), F32),
            V((LANES, LANES), F32),
            V((SLOTS, LANES), F32),
            V((np_, SLOTS, LANES), F32),
            V((1, LANES), jnp.int32),
            V((np_, 1, LANES), jnp.int32),
            pltpu.SMEM((np_, 1, LANES), jnp.int32),
            V((LANES, width), BF),
            V((80, width), F32),
            V((64, 256), BF),
            V((np_, rows, LANES), F32),
            V((np_, rows, LANES), F32),
            pltpu.SMEM((2, ql * np_), jnp.int32),
            V((512, 512), BF),
            V((width // 8, 512), BF),
            V((64, width), BF),
            V((np_, rows, width), F32),
            sem((2,)), sem((4,)), sem((14,)),
        ],
        compiler_params=pltpu.CompilerParams(collective_id=0, has_side_effects=True),
        name="self_energy",
    )(
        coupling.reshape(rl, 2048),
        eigvec.reshape(16, LANES),
        energies,
        k_coords,
        r_coords,
        degeneracy,
        kq_index,
        omega.T,
        jnp.transpose(phonon_modes, (1, 2, 0)).reshape(np_ * np_, ql),
    )


def solution(mesh):
    in_specs = (
        P("ka", "pb", None),
        P("ka", None),
        P("ka", None),
        P(),
        P(None, "ka"),
        P("ka"),
        P("ka", "pb"),
        P("pb", None),
        P("pb", None, None),
    )
    return jax.shard_map(
        functools.partial(shards, mesh), mesh=mesh, in_specs=in_specs,
        out_specs=P("ka", "pb"), check_vma=False)
```
